32 devices in a mesh: slab: 4 (over z), pencil: 8 (over y, x, core).
Axes of the slice: x: 2, y: 2, z: 4, core: 2. Of those that a mesh axis runs over, the one named last changes fastest.
Arguments:
- right_sides: float32 [8, 128, 128, 128], P(None, 'slab', 'pencil'), may hold values from -6 to 6
- spectrum: float32 [128, 128, 128], P('pencil', 'slab'), may hold values from 0.5 to 20, as said below
- noise_var: float32 [128, 128, 128], P('slab', 'pencil'), may hold values from 0.05 to 1
- observed: int32 [128, 128, 128], P('slab', 'pencil'), may hold values 0 or 1
Outputs:
- solution: float32 [8, 128, 128, 128], P(None, 'slab', 'pencil')
- noise_grad: float32 [128, 128, 128], P('slab', 'pencil')
The draws below stay inside these ranges and needn't reach their ends.
Inputs may be any that keep to these rules, and one draw needn't show every extreme that they name: Even in every index: spectrum[a, b, c] equals spectrum[(-a) mod 128, (-b) mod 128, (-c) mod 128].
All inputs are finite; a program needn't handle non-finite values. No bound on the sum of `observed` on one device may be relied on, other than what follows from the above.
Results may differ from the reference program's by a relative error of at most 0.00021.
Values sent between devices are 32-bit elements; how exact they have to be, the bound alone decides.
A program may use at most 128 MiB of HBM per device.

```python
import math
import jax
import jax.numpy as jnp
from jax import lax

NZ = 128
NY = 128
NX = 128
PROBES = 8
ITERS = 3


def draw_spectrum(key, part):
    base_values = jnp.exp(jax.random.uniform(key, (NX, NY, NZ), jnp.float32, math.log(0.5), math.log(20.0)))
    mirror = jnp.roll(jnp.flip(base_values, (0, 1, 2)), 1, (0, 1, 2))
    return 0.5 * (base_values + mirror)


def touch_ends(array, own_key, low, largest):
    extent = array.shape
    place = [jax.random.randint(jax.random.fold_in(own_key, axis), (), 0, extent[axis]) for axis in range(len(extent))]
    array = array.at[tuple(place)].set(low)
    longest = extent.index(max(extent))
    place[longest] = (place[longest] + 1) % extent[longest]
    return array.at[tuple(place)].set(largest)


def steps_of(own_key, extent, split, low, top_value):
    def one(position, parts):
        draws = jax.random.uniform(jax.random.fold_in(jax.random.fold_in(own_key, 6), position), (parts,), jnp.float32, low / len(split), top_value / len(split))
        return jnp.repeat(jnp.exp(draws), extent[position] // parts).reshape((-1,) + (1,) * (len(extent) - position - 1))

    factor_of = one(*split[0])
    for cut in split[1:]:
        factor_of = factor_of * one(*cut)
    return factor_of


def centred(rng, shape, deviation, reach, split=(), kind=jnp.bfloat16):
    factor_of = steps_of(rng, shape, split, -0.22, 0.18) if split else 1.0
    values = jax.random.normal(rng, shape, jnp.float32) * deviation * factor_of
    return jnp.minimum(jnp.maximum(values, -reach), reach).astype(kind)


def setup_inputs(seed: int = 0) -> dict:
    key_list = jax.random.split(jax.random.key(seed), 5)
    right_sides = centred(key_list[0], (PROBES, NZ, NY, NX), 1.0, 6.0, ((1, 4), (2, 8)), jnp.float32)
    spectrum = draw_spectrum(jax.random.fold_in(key_list[4], 71), 0)
    noise_var = jnp.clip(jnp.exp(math.log(1.0) - 2.9957323 * jax.random.uniform(key_list[2], (NZ, NY, NX), jnp.float32) ** steps_of(key_list[2], (NZ, NY, NX), ((0, 4), (1, 8)), -0.2, 0.2)), 0.05, 1.0)
    observed = touch_ends((jax.random.randint(key_list[3], (NZ, NY, NX), 0, 4) < 3).astype(jnp.int32), jax.random.fold_in(key_list[3], 1), 0, 1)
    return dict(right_sides=right_sides, spectrum=spectrum, noise_var=noise_var, observed=observed)


precise = lax.Precision.HIGHEST

def symmetric(matrix):
    return 0.5 * (matrix + matrix.T)

def solve_spd(matrix, right_hand):
    factor = jnp.linalg.cholesky(symmetric(matrix))
    halfway = lax.linalg.triangular_solve(factor, right_hand, left_side=True, lower=True)
    return lax.linalg.triangular_solve(factor, halfway, left_side=True, lower=True, transpose_a=True)

def gram_local(left, right):
    column_count = left.shape[0]
    return jnp.dot(left.reshape(column_count, -1), right.reshape(column_count, -1).T, precision=precise)

def combine(field_block, coefficients):
    column_count = field_block.shape[0]
    mixed = jnp.dot(coefficients.T, field_block.reshape(column_count, -1), precision=precise)
    return mixed.reshape(field_block.shape)

def operate(field_block, eigen_block, seen_cells, noise_var):
    masked = field_block * seen_cells
    spectral = jnp.fft.fftn(masked, axes=(1, 2, 3))
    smooth = jnp.real(jnp.fft.ifftn(spectral * eigen_block, axes=(1, 2, 3))).astype(jnp.float32)
    return seen_cells * smooth + noise_var * field_block

def reference(right_sides, spectrum, noise_var, observed):
    eigen_block = jnp.transpose(spectrum, (2, 1, 0))
    seen_cells = observed.astype(jnp.float32)
    solution = jnp.zeros_like(right_sides)
    residual = right_sides
    direction = right_sides
    gamma_now = gram_local(residual, residual)
    for iteration in range(ITERS):
        image_block = operate(direction, eigen_block, seen_cells, noise_var)
        delta_now = gram_local(direction, image_block)
        alpha_step = solve_spd(delta_now, gamma_now)
        solution = solution + combine(direction, alpha_step)
        if iteration + 1 < ITERS:
            residual = residual - combine(image_block, alpha_step)
            gamma_next = gram_local(residual, residual)
            beta_step = solve_spd(gamma_now, gamma_next)
            direction = residual + combine(direction, beta_step)
            gamma_now = gamma_next
    weights = right_sides[1:] * solution[1:]
    noise_grad = 0.5 * (solution[0] * solution[0] - jnp.mean(weights, axis=0))
    return (solution, noise_grad)
```

```python
import functools

import jax
import jax.numpy as jnp
import numpy as np
from jax import lax
from jax.experimental import pallas as pl
from jax.experimental.pallas import tpu as pltpu
from jax.sharding import PartitionSpec as P

ITERS = 3
SHIFT = 8.0
SCALE = 8.0
FLOOR = 3e-3
F32 = jnp.float32
BF16 = jnp.bfloat16
INTERPRET = False

precise = lax.Precision.HIGHEST


def embed(length, forward, scale=1.0):
    points = np.arange(length)
    angles = (points[:, None] * points[None, :] % length) * (2.0 * np.pi / length)
    cosine, sine = np.cos(angles) * scale, np.sin(angles) * scale
    if not forward:
        sine = -sine
    return np.block([[cosine, sine], [-sine, cosine]])


def halves(table):
    table = np.asarray(table, np.float32)
    high = table.astype(BF16)
    low = (table - high.astype(np.float32)).astype(BF16)
    return np.stack((high, low))


def split(values):
    high = values.astype(BF16)
    return high, (values - high.astype(F32)).astype(BF16)


def dot3(left, right, dims=((1,), (0,))):
    mul = functools.partial(
        lax.dot_general, dimension_numbers=(dims, ((), ())), preferred_element_type=F32
    )
    return mul(left[0], right[0]) + (mul(left[1], right[0]) + mul(left[0], right[1]))


def solve(matrix, right_hand):
    size = matrix.shape[0]
    both = jnp.concatenate((0.5 * (matrix + matrix.T), right_hand), axis=1)
    place = lax.broadcasted_iota(jnp.int32, both.shape, 0)
    for i in range(size):
        row = both[i : i + 1] / both[i : i + 1, i : i + 1]
        both = jnp.where(place == i, row, both - both[:, i : i + 1] * row)
    return both[:, size:]


def least_pivots(matrix):
    size = matrix.shape[0]
    both = 0.5 * (matrix + matrix.T)
    place = lax.broadcasted_iota(jnp.int32, both.shape, 0)
    lane = lax.broadcasted_iota(jnp.int32, both.shape, 1)
    for i in range(size):
        row = both[i : i + 1] / both[i : i + 1, i : i + 1]
        both = jnp.where(place > i, both - both[:, i : i + 1] * row, both)
    return jnp.sum(jnp.where(place == lane, both, 0.0), axis=0, keepdims=True)


def dot(left, right):
    return jnp.dot(left, right, precision=precise, preferred_element_type=F32)


def small(hankel):
    columns = hankel.shape[0] // (ITERS + 1)

    def operator(c):
        zero = jnp.zeros((columns, columns), F32)
        return SHIFT * c + SCALE * jnp.concatenate((zero, c[: ITERS * columns]), axis=0)

    def inner(u, v):
        return dot(u.T, dot(hankel, v))

    shape = (hankel.shape[0], columns)
    same = lax.broadcasted_iota(jnp.int32, shape, 0) == lax.broadcasted_iota(jnp.int32, shape, 1)
    residual = jnp.where(same, 1.0, 0.0).astype(F32)
    direction, answer = residual, jnp.zeros(shape, F32)
    gamma = hankel[:columns, :columns]
    start = least_pivots(gamma)
    fine = jnp.ones((1, columns), F32)
    for iteration in range(ITERS):
        image = operator(direction)
        alpha = solve(inner(direction, image), gamma)
        answer = answer + dot(direction, alpha)
        if iteration + 1 < ITERS:
            residual = residual - dot(image, alpha)
            gamma_next = inner(residual, residual)
            fine = jnp.where(least_pivots(gamma_next) > FLOOR * start, fine, 0.0)
            beta = solve(gamma, gamma_next)
            direction = residual + dot(direction, beta)
            gamma = gamma_next
    return answer, fine


def final_kernel(c_ref, p0, p1, p2, x_ref, g_ref):
    quads, ys, both, depth, _ = p0.shape
    columns = quads * both
    tile = min(8, depth)
    basis = (p0, p1, p2)
    for half in range(2):
        span = range(half * columns // 2, (half + 1) * columns // 2)
        mix = [[c_ref[k * columns + i, p] for p in span] for k in range(3) for i in range(columns)]

        def body(step, carry):
            y = step // (depth // tile)
            rows = pl.ds(pl.multiple_of(step % (depth // tile) * tile, tile), tile)
            sums = [0.0] * len(span)
            for k in range(3):
                for i in range(columns):
                    value = basis[k][i // both, y, i % both, rows]
                    sums = [s + value * m for s, m in zip(sums, mix[k * columns + i])]
            grad = 0.0
            for s, p in zip(sums, span):
                x_ref[p // both, y, p % both, rows] = s
                if p == 0:
                    grad = grad + 0.5 * s * s
                else:
                    grad = grad - p0[p // both, y, p % both, rows] * s * (0.5 / (columns - 1))
            g_ref[y, rows] = grad if half == 0 else g_ref[y, rows] + grad
            return carry

        lax.fori_loop(0, ys * (depth // tile), body, 0)


MESH = pl.DeviceIdType.MESH


class Group:
    def __init__(self, sizes, axis):
        self.axis, self.size = axis, sizes[axis]
        self.names = tuple(sizes)
        self.place = {name: lax.axis_index(name) for name in sizes}
        self.me = self.place[axis]

    def peer(self, step):
        return lax.rem(self.me + step, self.size)

    def device(self, other):
        return tuple(other if name == self.axis else self.place[name] for name in self.names)

    def copy(self, src, dst, send, recv, other):
        return pltpu.make_async_remote_copy(
            src_ref=src, dst_ref=dst, send_sem=send, recv_sem=recv,
            device_id=self.device(other), device_id_type=MESH,
        )


def greet(groups):
    barrier = pltpu.get_barrier_semaphore()
    total = 0
    for group in groups:
        for step in range(1, group.size):
            pl.semaphore_signal(
                barrier, inc=1, device_id=group.device(group.peer(step)), device_id_type=MESH
            )
            total += 1
    pl.semaphore_wait(barrier, total)


def spread(group, source, target, send, recv):
    copies = []
    for step in range(1, group.size):
        copy = group.copy(
            source, target.at[group.me], send.at[step], recv.at[step], group.peer(step)
        )
        copy.start()
        copies.append(copy)
    target[group.me] = source[...]
    for copy in copies:
        copy.wait()
    total = target[0]
    for place in range(1, group.size):
        total = total + target[place]
    return total


def total_kernel(sizes, v_ref, o_ref, part, one, two, send, recv, send2, recv2):
    slab, pencil = Group(sizes, "slab"), Group(sizes, "pencil")
    greet((slab, pencil))
    part[...] = spread(pencil, v_ref, one, send, recv)
    o_ref[...] = spread(slab, part, two, send2, recv2)


def total_scratch(sizes, shape):
    return [
        pltpu.VMEM(shape, F32),
        pltpu.VMEM((sizes["pencil"],) + shape, F32),
        pltpu.VMEM((sizes["slab"],) + shape, F32),
        pltpu.SemaphoreType.DMA((sizes["pencil"],)),
        pltpu.SemaphoreType.DMA((sizes["pencil"],)),
        pltpu.SemaphoreType.DMA((sizes["slab"],)),
        pltpu.SemaphoreType.DMA((sizes["slab"],)),
    ]


def total_of(matrix):
    if INTERPRET:
        return lax.psum(matrix, ("slab", "pencil"))
    sizes = {name: lax.axis_size(name) for name in ("slab", "pencil")}
    rows, columns = matrix.shape
    wide = jnp.pad(matrix, ((0, 0), (0, 128 - columns)))
    found = pl.pallas_call(
        functools.partial(total_kernel, sizes),
        in_specs=[pl.BlockSpec(memory_space=pltpu.VMEM)],
        out_specs=pl.BlockSpec(memory_space=pltpu.VMEM),
        out_shape=jax.ShapeDtypeStruct(wide.shape, F32),
        scratch_shapes=total_scratch(sizes, wide.shape),
        compiler_params=pltpu.CompilerParams(collective_id=1, has_side_effects=True),
    )(wide)
    return found[:, :columns]


def krylov_kernel(
    sizes, plan,
    wf, field, spectrum, noise, seen, fx_h, fz_h, gx_h, gz_h, fy_h, gy_h,
    p1_o, p2_o, u2_o, c_ref, ok_ref,
    w0, wa, x1, x2, x3, eig, noi, see, put, got, tmp, p0, nown, sown,
    fx, fz, gx, gz, fy, gy, rows, stat, part_sum, one, two,
    xsend, xrecv, xown, zsend, zrecv, zown, hsend, hrecv, lsem, s1, r1, s2, r2,
):
    slab, pencil = Group(sizes, "slab"), Group(sizes, "pencil")
    slabs, pencils = slab.size, pencil.size
    _, ys, _, depth, nx = w0.shape
    part, wide = got[0].shape[1], got[0].shape[3]
    nz = wide // 2
    chunk, block, piece, odd = plan
    chunks, blocks = ys // chunk, part // block
    columns = field.shape[0] * 2
    tile = min(8, depth)
    depths = depth // tile

    tables = ((fx_h, fx), (fz_h, fz), (gx_h, gx), (gz_h, gz), (fy_h, fy), (gy_h, gy))
    loads = [pltpu.make_async_copy(a, b, lsem.at[i]) for i, (a, b) in enumerate(
        tables + ((field, p0), (noise, nown), (seen, sown)))]
    for load in loads:
        load.start()
    greet((slab, pencil))

    def zrows(ref, y, count):
        return ref.at[:, pl.ds(y, count)]

    def zcopies(number, slot, y, count, src, dst):
        made = []
        for step in range(1, slabs):
            other = slab.peer(step)
            made.append(slab.copy(
                src.at[other, pl.ds(y, count)], dst.at[slab.me, pl.ds(y, count)],
                zsend.at[number, slot, step], zrecv.at[number, slot, step], other,
            ))
        made.append(pltpu.make_async_copy(
            src.at[slab.me, pl.ds(y, count)], dst.at[slab.me, pl.ds(y, count)],
            zown.at[number, slot],
        ))
        return made

    def start(copies):
        for copy in copies:
            copy.start()

    def finish(copies):
        for copy in copies:
            copy.wait()

    gathers = ((spectrum, eig), (noise, noi), (seen, see))

    def hop(number, stage):
        own, full = gathers[number]
        sems = lambda way: (hsend.at[number, stage, way], hrecv.at[number, stage, way])

        def send(way, origin, other):
            src = own if stage == 0 else full.at[origin]
            slab.copy(src, full.at[origin], *sems(way), other).start()

        @pl.when((slab.me + 1 < slabs) & (slab.me >= stage))
        def _():
            send(0, slab.me - stage, slab.me + 1)

        @pl.when((slab.me >= 1) & (slab.me + stage < slabs))
        def _():
            send(1, slab.me + stage, slab.me - 1)

    def landed(number, stage):
        own, full = gathers[number]
        for way, origin, ok in (
            (0, slab.me - 1 - stage, slab.me >= 1 + stage),
            (1, slab.me + 1 + stage, slab.me + 1 + stage < slabs),
        ):
            @pl.when(ok)
            def _():
                slab.copy(
                    own, full.at[origin], hsend.at[number, stage, way],
                    hrecv.at[number, stage, way], slab.peer(1),
                ).wait_recv()

    def left(number, stage):
        own, full = gathers[number]
        for way, ok in (
            (0, (slab.me + 1 < slabs) & (slab.me >= stage)),
            (1, (slab.me >= 1) & (slab.me + stage < slabs)),
        ):
            @pl.when(ok)
            def _():
                slab.copy(
                    own, full.at[slab.me], hsend.at[number, stage, way],
                    hrecv.at[number, stage, way], slab.peer(1),
                ).wait_send()

    def xcopy(number, slot, step, view):
        other = pencil.peer(step)
        return pencil.copy(
            view(put[number % 2], other), view(got[number], pencil.me),
            xsend.at[number, slot, step], xrecv.at[number, slot, step], other,
        )

    def xself(number, slot, view):
        return pltpu.make_async_copy(
            view(put[number % 2], pencil.me), view(got[number], pencil.me), xown.at[number, slot]
        )

    def by_rows(c):
        return lambda ref, place: ref.at[place, :, pl.ds(c * chunk, chunk)]

    def by_part(b):
        return lambda ref, place: ref.at[place, pl.ds(b * block, block)]

    def xfinish(number, slots, view):
        for slot in range(slots):
            for step in range(1, pencils):
                xcopy(number, slot, step, view(slot)).wait()
            xself(number, slot, view(slot)).wait()

    def first_stage(j, real, imag):
        length = real.shape[1]
        data = split(jnp.concatenate((real, imag), axis=1))
        first = dot3((fx[0], fx[1]), data, ((1,), (1,)))
        first = jnp.concatenate((first[:length], first[length:]), axis=1)
        for q in range(pencils):
            tmp[j, q] = first[q * part : (q + 1) * part]

    def emit(number, c):
        span = pl.ds(c * chunk, chunk)

        def one_block(q):
            data = jnp.concatenate([tmp[j, q] for j in range(chunk)], axis=0)
            out = dot3(split(data), (fz[0], fz[1]))
            out = jnp.stack([out[j * part : (j + 1) * part] for j in range(chunk)])
            put[number % 2][q, :, span] = jnp.swapaxes(out, 0, 1)

        def body(step, carry):
            one_block(pencil.peer(step))
            xcopy(number, c, step, by_rows(c)).start()
            return carry

        lax.fori_loop(1, pencils, body, 0)
        one_block(pencil.me)
        xself(number, c, by_rows(c)).start()

    def absorb(number, c):
        span = pl.ds(c * chunk, chunk)

        def body(q, carry):
            data = jnp.swapaxes(got[number][q, :, span], 0, 1)
            data = jnp.concatenate([data[j] for j in range(chunk)], axis=0)
            out = dot3(split(data), (gz[0], gz[1]))
            for j in range(chunk):
                tmp[j, q] = out[j * part : (j + 1) * part]
            return carry

        lax.fori_loop(0, pencils, body, 0)

    def plane_back(j):
        first = jnp.concatenate([tmp[j, q] for q in range(pencils)], axis=0)
        first = jnp.concatenate((first[:, :nz], first[:, nz:]), axis=0)
        plane = dot3(split(first), (gx[0], gx[1]), ((0,), (0,)))
        return plane[:, :nx], plane[:, nx:]

    def lines(ref, y):
        return jnp.concatenate([ref[s, y] for s in range(slabs)], axis=0)

    def plane(ref, y, c):
        return jnp.concatenate([ref[s, y, c] for s in range(slabs)], axis=0)

    def store(ref, y, values):
        for c in range(2):
            for s in range(slabs):
                ref[s, y, c] = values[c][s * depth : (s + 1) * depth]

    def middle(number, after=None):
        def body(b, carry):
            for a2 in range(0, block, 2):
                spots = range(a2, min(a2 + 2, block))
                halves_of = []
                for a in spots:
                    data = jnp.concatenate(
                        [got[number][q, b * block + a] for q in range(pencils)], axis=0)
                    halves_of.append(jnp.concatenate((data[:, :nz], data[:, nz:]), axis=0))
                spec = dot3((fy[0], fy[1]), split(jnp.concatenate(halves_of, axis=1)))
                eigen = jnp.concatenate([
                    jnp.concatenate([eig[s, b * block + a] for s in range(slabs)], axis=0)
                    for a in spots], axis=1)
                spec = spec * jnp.concatenate((eigen, eigen), axis=0)
                back = dot3((gy[0], gy[1]), split(spec))
                ny = back.shape[0] // 2
                for k, a in enumerate(spots):
                    mine = back[:, k * nz : (k + 1) * nz]
                    mine = jnp.concatenate((mine[:ny], mine[ny:]), axis=1)
                    for q in range(pencils):
                        put[(number + 1) % 2][q, b * block + a] = mine[q * ys : (q + 1) * ys]
            for step in range(1, pencils):
                xcopy(number + 1, b, step, by_part(b)).start()
            xself(number + 1, b, by_part(b)).start()
            return carry

        lax.fori_loop(0, blocks, body, 0)

    def advance(number, old, new, target, which):
        for c in range(chunks):
            absorb(number, c)

            def body(j, carry):
                y = c * chunk + j
                found = plane_back(j)
                mask, shift = lines(see, y), lines(noi, y) - SHIFT
                values = tuple(
                    (mask * t + shift * plane(old, y, k)) * (1.0 / SCALE)
                    for k, t in enumerate(found)
                )
                store(new, y, values)
                first_stage(j, *values)
                return carry

            lax.fori_loop(0, chunk, body, 0)
            emit(number + 1, c)
            start(zcopies(which, c, c * chunk, chunk, new, target))

    pieces = ys // piece
    for k in range(pieces):
        start(zcopies(0, k, k * piece, piece, wf, w0))
    own_loads = [pltpu.make_async_copy(own, full.at[slab.me], lsem.at[len(loads) + i])
                 for i, (own, full) in enumerate(gathers)]
    start(own_loads)
    hop(0, 0)
    for load in loads[:6]:
        load.wait()
    for c in range(chunks):
        for k in range(c * chunk // piece, (c + 1) * chunk // piece):
            finish(zcopies(0, k, k * piece, piece, wf, w0))

            def enter(j, carry):
                y = k * piece + j
                first_stage(y - c * chunk, plane(w0, y, 0), plane(w0, y, 1))
                return carry

            lax.fori_loop(0, piece, enter, 0)
        emit(0, c)
    for stage in range(slabs - 1):
        landed(0, stage)
        if stage + 2 < slabs:
            hop(0, stage + 1)
        if stage == 0:
            hop(1, 0)
            hop(2, 0)
    finish(own_loads)
    xfinish(0, chunks, by_rows)
    middle(0)
    for stage in range(slabs - 1):
        for number in (1, 2):
            landed(number, stage)
            if stage + 2 < slabs:
                hop(number, stage + 1)
    xfinish(1, blocks, by_part)
    advance(1, w0, wa, x1, 1)
    xfinish(2, chunks, by_rows)
    middle(2)
    xfinish(3, blocks, by_part)
    advance(3, wa, w0, x2, 2)
    xfinish(4, chunks, by_rows)
    middle(4)
    for c in range(chunks):
        finish(zcopies(1, c, c * chunk, chunk, wa, x1))
    xfinish(5, blocks, by_part)
    for c in range(chunks):
        absorb(5, c)

        def leave(j, carry):
            store(wa, c * chunk + j, plane_back(j))
            return carry

        lax.fori_loop(0, chunk, leave, 0)
        start(zcopies(3, c, c * chunk, chunk, wa, x3))

    def spot(ref, i, y, z):
        return (ref, (i, y, 0, z) if odd else (i // 2, y, i % 2, z))

    def tiles(step, c):
        y = c * chunk + step // depths
        return y, pl.ds(pl.multiple_of(step % depths * tile, tile), tile)

    pairs = [(i, j) for i in range(columns) for j in range(i, columns)]
    zero = tuple(jnp.zeros((tile, nx), F32) for _ in pairs)
    lane = lax.broadcasted_iota(jnp.int32, stat.shape, 1)

    def at(ref, i, y, z):
        return ref[i, y, 0, z] if odd else ref[i // 2, y, i % 2, z]

    def base(ref, i, y, z):
        return ref[i // 2, y, i % 2, z]

    def note(moment, sums):
        for total, (i, j) in zip(sums, pairs):
            row = jnp.sum(total, axis=0, keepdims=True)
            rows[pl.ds(i * columns + j, 1)] = row
            if i != j:
                rows[pl.ds(j * columns + i, 1)] = row
        found = stat[...]
        for i in range(columns):
            column = jnp.sum(rows[pl.ds(i * columns, columns)], axis=1, keepdims=True)
            found = jnp.where(lane == moment * columns + i, column, found)
        stat[...] = found

    def moment(number, left_of, right_of):
        def body(step, sums):
            y, z = tiles(step, 0)
            lefts = [left_of(i, y, z) for i in range(columns)]
            rights = lefts if right_of is left_of else [right_of(i, y, z) for i in range(columns)]
            return tuple(s + lefts[i] * rights[j] for s, (i, j) in zip(sums, pairs))

        note(number, lax.fori_loop(0, ys * depths, body, zero))

    stat[...] = jnp.zeros(stat.shape, F32)
    for load in loads[6:]:
        load.wait()
    for c in range(chunks):
        finish(zcopies(2, c, c * chunk, chunk, w0, x2))

    def shape_basis(step, carry):
        y, z = tiles(step, 0)
        mask = sown[y, z] > 0
        factor = (nown[y, z] - SHIFT) * (1.0 / SCALE)
        for i in range(columns):
            once = factor * base(p0, i, y, z)
            place = (i, y, 0, z) if odd else (i // 2, y, i % 2, z)
            x1[place] = jnp.where(mask, x1[place], once)
            x2[place] = jnp.where(mask, x2[place], factor * once)
        return carry

    lax.fori_loop(0, ys * depths, shape_basis, 0)
    outs = [pltpu.make_async_copy(x1, p1_o, lsem.at[0]), pltpu.make_async_copy(x2, p2_o, lsem.at[1])]
    start(outs)
    of0, of1, of2 = (functools.partial(f, r) for f, r in ((base, p0), (at, x1), (at, x2)))
    for number, (l, r) in enumerate(((of0, of0), (of0, of1), (of1, of1), (of1, of2), (of2, of2))):
        moment(number, l, r)
    sums = zero
    for c in range(chunks):
        finish(zcopies(3, c, c * chunk, chunk, wa, x3))

        def last(step, sums):
            y, z = tiles(step, c)
            mask = sown[y, z] * (1.0 / SCALE)
            factor = (nown[y, z] - SHIFT) * (1.0 / SCALE)
            lefts, rights = [], []
            for i in range(columns):
                place = (i, y, 0, z) if odd else (i // 2, y, i % 2, z)
                lefts.append(x2[place])
                rights.append(mask * x3[place] + factor * lefts[-1])
                x3[place] = rights[-1]
            return tuple(s + lefts[i] * rights[j] for s, (i, j) in zip(sums, pairs))

        sums = lax.fori_loop(0, chunk * depths, last, sums)
    note(5, sums)
    out = pltpu.make_async_copy(x3, u2_o, lsem.at[2])
    out.start()
    for number in range(len(gathers)):
        for stage in range(slabs - 1):
            left(number, stage)
    part_sum[...] = spread(pencil, stat, one, s1, r1)
    found = spread(slab, part_sum, two, s2, r2)
    hankel = jnp.concatenate(
        [found[:, j * columns : (j + ITERS + 1) * columns] for j in range(ITERS + 1)], axis=0)
    c_ref[...], ok_ref[...] = small(hankel)
    finish(outs)
    out.wait()


def krylov(wf, field, spectrum, noise, seen, tables):
    sizes = {name: lax.axis_size(name) for name in ("slab", "pencil")}
    slabs, pencils = sizes["slab"], sizes["pencil"]
    quads, ys, _, depth, nx = field.shape
    columns = 2 * quads
    part, below, nz = spectrum.shape
    wide = 2 * nz
    chunk = 8 if ys % 8 == 0 else ys
    block = min(4, part)
    piece = min(4, chunk)
    planes = (slabs, ys, 2, depth, nx)
    gathered = (slabs, ys, depth, nx)
    sent = (pencils, part, ys, wide)
    slots = max(ys // chunk, part // block)
    any_space = pl.BlockSpec(memory_space=pl.ANY)
    vmem = pl.BlockSpec(memory_space=pltpu.VMEM)
    dma = pltpu.SemaphoreType.DMA
    tile = (columns, 128)
    scratch = (
        [pltpu.VMEM(planes, F32)] * 5
        + [pltpu.VMEM((slabs,) + spectrum.shape, F32)]
        + [pltpu.VMEM(gathered, F32)] * 2
        + [[pltpu.VMEM(sent, F32)] * 2, [pltpu.VMEM(sent, F32)] * 6]
        + [pltpu.VMEM((chunk, pencils, part, wide), F32), pltpu.VMEM(field.shape, F32)]
        + [pltpu.VMEM(noise.shape, F32)] * 2
        + [pltpu.VMEM(t.shape, BF16) for t in tables]
        + [pltpu.VMEM((columns * columns, nx), F32), pltpu.VMEM(tile, F32)]
        + total_scratch(sizes, tile)[:3]
        + [dma((6, slots, pencils))] * 2 + [dma((6, slots))]
        + [dma((4, ys // piece, slabs))] * 2 + [dma((4, ys // piece))]
        + [dma((3, slabs, 2))] * 2 + [dma((12,))]
        + total_scratch(sizes, tile)[3:]
    )
    return pl.pallas_call(
        functools.partial(krylov_kernel, sizes, (chunk, block, piece, slabs == columns)),
        in_specs=[any_space] * 11,
        out_specs=(any_space, any_space, any_space, vmem, vmem),
        out_shape=(jax.ShapeDtypeStruct(planes, F32),) * 3 + (
            jax.ShapeDtypeStruct(((ITERS + 1) * columns, columns), F32),
            jax.ShapeDtypeStruct((1, columns), F32),
        ),
        scratch_shapes=scratch,
        cost_estimate=pl.CostEstimate(flops=2**33, bytes_accessed=2**26, transcendentals=0),
        compiler_params=pltpu.CompilerParams(
            collective_id=0, has_side_effects=True, vmem_limit_bytes=60 * 2**20
        ),
    )(wf, field, spectrum, noise, seen, *tables)


def recurrences(p0, p1, p2, u2):
    flat = lambda v: jnp.swapaxes(v, 1, 2).reshape(v.shape[0] * v.shape[2], -1)
    basis = [flat(v) for v in (p0, p1, p2, u2)]
    columns = basis[0].shape[0]

    def field(c):
        return sum(dot(c[k].T, basis[k]) for k in range(len(c)))

    def gram(u, v):
        return total_of(jnp.dot(u, v.T, precision=precise))

    def operator(c):
        zero = jnp.zeros((1, columns, columns), F32)
        return SHIFT * jnp.concatenate((c, zero)) + SCALE * jnp.concatenate((zero, c))

    def longer(c):
        return jnp.concatenate((c, jnp.zeros((1, columns, columns), F32)))

    residual = direction = answer = jnp.eye(columns, dtype=F32)[None]
    answer = 0.0 * answer
    vector = field(residual)
    gamma = gram(vector, vector)
    for iteration in range(ITERS):
        image = operator(direction)
        alpha = solve(gram(field(direction), field(image)), gamma)
        answer = answer + jnp.einsum("kij,jp->kip", direction, alpha, precision=precise)
        if iteration + 1 < ITERS:
            residual = longer(residual) - jnp.einsum("kij,jp->kip", image, alpha, precision=precise)
            vector = field(residual)
            gamma_next = gram(vector, vector)
            beta = solve(gamma, gamma_next)
            direction = residual + longer(
                jnp.einsum("kij,jp->kip", direction, beta, precision=precise)
            )
            answer = longer(answer)
            gamma = gamma_next
    return answer.reshape(-1, columns)


def local(right_sides, spectrum, noise_var, observed):
    columns, depth, ys, nx = right_sides.shape
    slabs, pencils = lax.axis_size("slab"), lax.axis_size("pencil")
    nz, ny = depth * slabs, ys * pencils
    seen = jnp.swapaxes(observed.astype(F32), 0, 1)
    noise = jnp.swapaxes(noise_var, 0, 1)
    quads = columns // 2
    field = jnp.transpose(right_sides.reshape(quads, 2, depth, ys, nx), (0, 3, 1, 2, 4))
    odd = columns // slabs % 2

    fx, gx = halves(embed(nx, True)), halves(embed(nx, False).T)
    fz, gz = halves(embed(nz, True).T), halves(embed(nz, False).T)
    fy, gy = halves(embed(ny, True)), halves(embed(ny, False, 1.0 / (nx * ny * nz)))
    tables = [jnp.asarray(t) for t in (fx, fz, gx, gz, fy, gy)]

    masked = field * seen[None, :, None]
    if odd:
        masked = jnp.swapaxes(masked, 1, 2).reshape(columns, ys, 1, depth, nx)
        masked = jnp.concatenate((masked, jnp.zeros_like(masked)), axis=2)
    *basis, coefficients, fine = krylov(masked, field, spectrum, noise, seen, tables)
    if odd:
        basis = [
            jnp.swapaxes(v[:, :, 0].reshape(quads, 2, ys, depth, nx), 1, 2) for v in basis
        ]
    p1, p2, u2 = basis
    coefficients = lax.cond(
        jnp.min(fine) > 0.5,
        lambda: coefficients[: 3 * columns],
        lambda: recurrences(field, p1, p2, u2),
    )
    answer, grad = pl.pallas_call(
        final_kernel,
        in_specs=[pl.BlockSpec(memory_space=pltpu.SMEM)]
        + [pl.BlockSpec(memory_space=pltpu.VMEM)] * 3,
        out_shape=(
            jax.ShapeDtypeStruct(field.shape, F32),
            jax.ShapeDtypeStruct((ys, depth, nx), F32),
        ),
        interpret=INTERPRET,
    )(coefficients, field, p1, p2)
    answer = jnp.transpose(answer, (0, 2, 3, 1, 4)).reshape(columns, depth, ys, nx)
    return answer, jnp.swapaxes(grad, 0, 1)


def solution(mesh):
    in_specs = (
        P(None, "slab", "pencil", None),
        P("pencil", "slab", None),
        P("slab", "pencil", None),
        P("slab", "pencil", None),
    )
    out_specs = (P(None, "slab", "pencil", None), P("slab", "pencil", None))
    return jax.shard_map(local, mesh=mesh, in_specs=in_specs, out_specs=out_specs, check_vma=False)
```

```python
import functools

import jax
import jax.numpy as jnp
import numpy as np
from jax import lax
from jax.experimental import pallas as pl
from jax.experimental.pallas import tpu as pltpu
from jax.sharding import PartitionSpec as P

ITERS = 3
SHIFT = 8.0
SCALE = 8.0
FLOOR = 3e-3
F32 = jnp.float32
BF16 = jnp.bfloat16
INTERPRET = False

precise = lax.Precision.HIGHEST


def embed(length, forward, scale=1.0):
    points = np.arange(length)
    angles = (points[:, None] * points[None, :] % length) * (2.0 * np.pi / length)
    cosine, sine = np.cos(angles) * scale, np.sin(angles) * scale
    if not forward:
        sine = -sine
    return np.block([[cosine, sine], [-sine, cosine]])


def halves(table):
    table = np.asarray(table, np.float32)
    high = table.astype(BF16)
    low = (table - high.astype(np.float32)).astype(BF16)
    return np.stack((high, low))


def split(values):
    high = values.astype(BF16)
    return high, (values - high.astype(F32)).astype(BF16)


def dot3(left, right, dims=((1,), (0,))):
    mul = functools.partial(
        lax.dot_general, dimension_numbers=(dims, ((), ())), preferred_element_type=F32
    )
    return mul(left[0], right[0]) + (mul(left[1], right[0]) + mul(left[0], right[1]))


def solve(matrix, right_hand):
    size = matrix.shape[0]
    both = jnp.concatenate((0.5 * (matrix + matrix.T), right_hand), axis=1)
    place = lax.broadcasted_iota(jnp.int32, both.shape, 0)
    for i in range(size):
        row = both[i : i + 1] / both[i : i + 1, i : i + 1]
        both = jnp.where(place == i, row, both - both[:, i : i + 1] * row)
    return both[:, size:]


def least_pivots(matrix):
    size = matrix.shape[0]
    both = 0.5 * (matrix + matrix.T)
    place = lax.broadcasted_iota(jnp.int32, both.shape, 0)
    lane = lax.broadcasted_iota(jnp.int32, both.shape, 1)
    for i in range(size):
        row = both[i : i + 1] / both[i : i + 1, i : i + 1]
        both = jnp.where(place > i, both - both[:, i : i + 1] * row, both)
    return jnp.sum(jnp.where(place == lane, both, 0.0), axis=0, keepdims=True)


def dot(left, right):
    return jnp.dot(left, right, precision=precise, preferred_element_type=F32)


def small(hankel):
    columns = hankel.shape[0] // (ITERS + 1)

    def operator(c):
        zero = jnp.zeros((columns, columns), F32)
        return SHIFT * c + SCALE * jnp.concatenate((zero, c[: ITERS * columns]), axis=0)

    def inner(u, v):
        return dot(u.T, dot(hankel, v))

    shape = (hankel.shape[0], columns)
    same = lax.broadcasted_iota(jnp.int32, shape, 0) == lax.broadcasted_iota(jnp.int32, shape, 1)
    residual = jnp.where(same, 1.0, 0.0).astype(F32)
    direction, answer = residual, jnp.zeros(shape, F32)
    gamma = hankel[:columns, :columns]
    start = least_pivots(gamma)
    fine = jnp.ones((1, columns), F32)
    for iteration in range(ITERS):
        image = operator(direction)
        alpha = solve(inner(direction, image), gamma)
        answer = answer + dot(direction, alpha)
        if iteration + 1 < ITERS:
            residual = residual - dot(image, alpha)
            gamma_next = inner(residual, residual)
            fine = jnp.where(least_pivots(gamma_next) > FLOOR * start, fine, 0.0)
            beta = solve(gamma, gamma_next)
            direction = residual + dot(direction, beta)
            gamma = gamma_next
    return answer, fine


def final_kernel(odd, c_ref, right, p1, p2, x_ref, g_ref):
    columns, tile, ys, _ = right.shape
    chunk = 8 if ys % 8 == 0 else ys

    def at(ref, i, y):
        return ref[i, pl.ds(y, chunk), 0] if odd else ref[i // 2, pl.ds(y, chunk), i % 2]

    for y in range(0, ys, chunk):
        rows = pl.ds(y, chunk)

        def column(p):
            found = 0.0
            for k, ref in ((1, p1), (2, p2)):
                for i in range(columns):
                    found = found + at(ref, i, y) * c_ref[k * columns + i, p]
            found = jnp.swapaxes(found, 0, 1)
            for i in range(columns):
                found = found + right[i, :, rows] * c_ref[i, p]
            x_ref[p, :, rows] = found
            return found

        def body(p, grad):
            return grad - right[p, :, rows] * column(p) * (0.5 / (columns - 1))

        first = column(0)
        g_ref[:, rows] = lax.fori_loop(1, columns, body, 0.5 * first * first)


QU, YU = 4, 4
MESH = pl.DeviceIdType.MESH


class Group:
    def __init__(self, sizes, axis):
        self.axis, self.size = axis, sizes[axis]
        self.names = tuple(sizes)
        self.place = {name: lax.axis_index(name) for name in sizes}
        self.me = self.place[axis]

    def peer(self, step):
        return lax.rem(self.me + step, self.size)

    def device(self, other):
        return tuple(other if name == self.axis else self.place[name] for name in self.names)

    def copy(self, src, dst, send, recv, other):
        return pltpu.make_async_remote_copy(
            src_ref=src, dst_ref=dst, send_sem=send, recv_sem=recv,
            device_id=self.device(other), device_id_type=MESH,
        )


def greet(groups):
    barrier = pltpu.get_barrier_semaphore()
    total = 0
    for group in groups:
        for step in range(1, group.size):
            pl.semaphore_signal(
                barrier, inc=1, device_id=group.device(group.peer(step)), device_id_type=MESH
            )
            total += 1
    pl.semaphore_wait(barrier, total)


def spread(group, source, target, send, recv):
    copies = []
    for step in range(1, group.size):
        copy = group.copy(
            source, target.at[group.me], send.at[step], recv.at[step], group.peer(step)
        )
        copy.start()
        copies.append(copy)
    target[group.me] = source[...]
    for copy in copies:
        copy.wait()
    total = target[0]
    for place in range(1, group.size):
        total = total + target[place]
    return total


def total_kernel(sizes, v_ref, o_ref, part, one, two, send, recv, send2, recv2):
    slab, pencil = Group(sizes, "slab"), Group(sizes, "pencil")
    greet((slab, pencil))
    part[...] = spread(pencil, v_ref, one, send, recv)
    o_ref[...] = spread(slab, part, two, send2, recv2)


def total_scratch(sizes, shape):
    return [
        pltpu.VMEM(shape, F32),
        pltpu.VMEM((sizes["pencil"],) + shape, F32),
        pltpu.VMEM((sizes["slab"],) + shape, F32),
        pltpu.SemaphoreType.DMA((sizes["pencil"],)),
        pltpu.SemaphoreType.DMA((sizes["pencil"],)),
        pltpu.SemaphoreType.DMA((sizes["slab"],)),
        pltpu.SemaphoreType.DMA((sizes["slab"],)),
    ]


def total_of(matrix):
    if INTERPRET:
        return lax.psum(matrix, ("slab", "pencil"))
    sizes = {name: lax.axis_size(name) for name in ("slab", "pencil")}
    rows, columns = matrix.shape
    wide = jnp.pad(matrix, ((0, 0), (0, 128 - columns)))
    found = pl.pallas_call(
        functools.partial(total_kernel, sizes),
        in_specs=[pl.BlockSpec(memory_space=pltpu.VMEM)],
        out_specs=pl.BlockSpec(memory_space=pltpu.VMEM),
        out_shape=jax.ShapeDtypeStruct(wide.shape, F32),
        scratch_shapes=total_scratch(sizes, wide.shape),
        compiler_params=pltpu.CompilerParams(collective_id=1, has_side_effects=True),
    )(wide)
    return found[:, :columns]


def krylov_kernel(
    sizes, plan,
    right, spectrum, noise, seen, fx_h, fz_h, gx_h, gz_h, fy_h, gy_h,
    p1_o, p2_o, u2_o, c_ref, ok_ref,
    w0, wa, x1, x2, x3, eig, noi, see, put, got, tmp, p0, nown, sown, nat, nnat, snat,
    fx, fz, gx, gz, fy, gy, rows, stat, part_sum, one, two,
    xsend, xrecv, xown, zsend, zrecv, zown, hsend, hrecv, lsem, s1, r1, s2, r2,
):
    slab, pencil = Group(sizes, "slab"), Group(sizes, "pencil")
    slabs, pencils = slab.size, pencil.size
    _, ys, _, depth, nx = w0.shape
    part, wide = got[0].shape[1], got[0].shape[3]
    nz = wide // 2
    chunk, block, piece, odd, enter_groups, groups = plan
    chunks, blocks = ys // chunk, part // block
    columns = right.shape[0]
    tile = min(8, depth)
    depths = depth // tile

    def brought(slot, src, dst):
        return pltpu.make_async_copy(src, dst, lsem.at[slot])

    naturals = []
    for c in range(chunks):
        span = pl.ds(c * chunk, chunk)
        naturals.append([
            brought(4 * c, seen.at[:, span], snat.at[:, span]),
            brought(4 * c + 1, right.at[:, :, span], nat.at[:, :, span]),
            brought(4 * c + 2, noise.at[:, span], nnat.at[:, span]),
        ])
        for load in naturals[-1]:
            load.start()
    tables = ((fx_h, fx), (fz_h, fz), (gx_h, gx), (gz_h, gz), (fy_h, fy), (gy_h, gy))
    loads = [brought(4 * chunks + i, a, b) for i, (a, b) in enumerate(tables)]
    for load in loads:
        load.start()
    greet((slab, pencil))

    def zrows(ref, y, count):
        return ref.at[:, pl.ds(y, count)]

    def zcopies(number, slot, y, count, src, dst):
        made = []
        for step in range(1, slabs):
            other = slab.peer(step)
            made.append(slab.copy(
                src.at[other, pl.ds(y, count)], dst.at[slab.me, pl.ds(y, count)],
                zsend.at[number, slot, step], zrecv.at[number, slot, step], other,
            ))
        made.append(pltpu.make_async_copy(
            src.at[slab.me, pl.ds(y, count)], dst.at[slab.me, pl.ds(y, count)],
            zown.at[number, slot],
        ))
        return made

    def start(copies):
        for copy in copies:
            copy.start()

    def finish(copies):
        for copy in copies:
            copy.wait()

    gathers = [(spectrum, lambda place: eig.at[place])]
    for c in range(chunks):
        span = pl.ds(c * chunk, chunk)
        for own, full in ((nown, noi), (sown, see)):
            gathers.append((
                own.at[span],
                functools.partial(lambda full, span, place: full.at[place, span], full, span),
            ))
    stages = [0] * len(gathers)

    def hop(number, stage):
        own, full = gathers[number]
        sems = lambda way: (hsend.at[number, stage, way], hrecv.at[number, stage, way])

        def send(way, origin, other):
            src = own if stage == 0 else full(origin)
            slab.copy(src, full(origin), *sems(way), other).start()

        @pl.when((slab.me + 1 < slabs) & (slab.me >= stage))
        def _():
            send(0, slab.me - stage, slab.me + 1)

        @pl.when((slab.me >= 1) & (slab.me + stage < slabs))
        def _():
            send(1, slab.me + stage, slab.me - 1)

    def halted(number, stage, way):
        own, full = gathers[number]
        return slab.copy(
            own, full(slab.me), hsend.at[number, stage, way], hrecv.at[number, stage, way],
            slab.peer(1),
        )

    def landed(number, stage):
        @pl.when(slab.me >= 1 + stage)
        def _():
            halted(number, stage, 0).wait_recv()

        @pl.when(slab.me + 1 + stage < slabs)
        def _():
            halted(number, stage, 1).wait_recv()

    def left(number, stage):
        @pl.when((slab.me + 1 < slabs) & (slab.me >= stage))
        def _():
            halted(number, stage, 0).wait_send()

        @pl.when((slab.me >= 1) & (slab.me + stage < slabs))
        def _():
            halted(number, stage, 1).wait_send()

    def relay(*numbers):
        for number in numbers:
            stage = stages[number]
            if stage + 1 < slabs:
                landed(number, stage)
                if stage + 2 < slabs:
                    hop(number, stage + 1)
                stages[number] = stage + 1

    def complete(*numbers):
        for _ in range(slabs - 1):
            relay(*numbers)

    def of_rows(c):
        return (1 + 2 * c, 2 + 2 * c)

    def xcopy(number, slot, step, view):
        other = pencil.peer(step)
        return pencil.copy(
            view(put[number % 2], other), view(got[number], pencil.me),
            xsend.at[number, slot, step], xrecv.at[number, slot, step], other,
        )

    def xself(number, slot, view):
        return pltpu.make_async_copy(
            view(put[number % 2], pencil.me), view(got[number], pencil.me), xown.at[number, slot]
        )

    def by_rows(group):
        return lambda ref, place: ref.at[place, :, pl.ds(*group)]

    def by_part(b):
        return lambda ref, place: ref.at[place, pl.ds(b * block, block)]

    def xfinish(number, views):
        for slot, view in enumerate(views):
            for step in range(1, pencils):
                xcopy(number, slot, step, view).wait()
            xself(number, slot, view).wait()

    def first_stage(j, real, imag):
        length = real.shape[1]
        data = split(jnp.concatenate((real, imag), axis=1))
        first = dot3((fx[0], fx[1]), data, ((1,), (1,)))
        first = jnp.concatenate((first[:length], first[length:]), axis=1)
        for q in range(pencils):
            tmp[j, q] = first[q * part : (q + 1) * part]

    def emit(number, slot, group):
        span, count = pl.ds(*group), group[1]

        def one_block(q):
            data = jnp.concatenate([tmp[j, q] for j in range(count)], axis=0)
            out = dot3(split(data), (fz[0], fz[1]))
            out = jnp.stack([out[j * part : (j + 1) * part] for j in range(count)])
            put[number % 2][q, :, span] = jnp.swapaxes(out, 0, 1)

        def body(step, carry):
            one_block(pencil.peer(step))
            xcopy(number, slot, step, by_rows(group)).start()
            return carry

        lax.fori_loop(1, pencils, body, 0, unroll=QU)
        one_block(pencil.me)
        xself(number, slot, by_rows(group)).start()

    def absorb(number, group):
        span, count = pl.ds(*group), group[1]

        def body(q, carry):
            data = jnp.swapaxes(got[number][q, :, span], 0, 1)
            data = jnp.concatenate([data[j] for j in range(count)], axis=0)
            out = dot3(split(data), (gz[0], gz[1]))
            for j in range(count):
                tmp[j, q] = out[j * part : (j + 1) * part]
            return carry

        lax.fori_loop(0, pencils, body, 0, unroll=QU)

    def plane_back(j):
        first = jnp.concatenate([tmp[j, q] for q in range(pencils)], axis=0)
        first = jnp.concatenate((first[:, :nz], first[:, nz:]), axis=0)
        plane = dot3(split(first), (gx[0], gx[1]), ((0,), (0,)))
        return plane[:, :nx], plane[:, nx:]

    def lines(ref, y):
        return jnp.concatenate([ref[s, y] for s in range(slabs)], axis=0)

    def plane(ref, y, c):
        return jnp.concatenate([ref[s, y, c] for s in range(slabs)], axis=0)

    def store(ref, y, values):
        for c in range(2):
            for s in range(slabs):
                ref[s, y, c] = values[c][s * depth : (s + 1) * depth]

    def middle(number, after=None):
        def body(b, carry):
            for a2 in range(0, block, 2):
                spots = range(a2, min(a2 + 2, block))
                halves_of = []
                for a in spots:
                    data = jnp.concatenate(
                        [got[number][q, b * block + a] for q in range(pencils)], axis=0)
                    halves_of.append(jnp.concatenate((data[:, :nz], data[:, nz:]), axis=0))
                spec = dot3((fy[0], fy[1]), split(jnp.concatenate(halves_of, axis=1)))
                eigen = jnp.concatenate([
                    jnp.concatenate([eig[s, b * block + a] for s in range(slabs)], axis=0)
                    for a in spots], axis=1)
                spec = spec * jnp.concatenate((eigen, eigen), axis=0)
                back = dot3((gy[0], gy[1]), split(spec))
                ny = back.shape[0] // 2
                for k, a in enumerate(spots):
                    mine = back[:, k * nz : (k + 1) * nz]
                    mine = jnp.concatenate((mine[:ny], mine[ny:]), axis=1)
                    for q in range(pencils):
                        put[(number + 1) % 2][q, b * block + a] = mine[q * ys : (q + 1) * ys]
            for step in range(1, pencils):
                xcopy(number + 1, b, step, by_part(b)).start()
            xself(number + 1, b, by_part(b)).start()
            return carry

        lax.fori_loop(0, blocks, body, 0)

    def advance(number, old, new, target, which, ready=None):
        for slot, group in enumerate(groups):
            start_row, count = group
            absorb(number, group)
            if ready is not None:
                ready(start_row // chunk)

            def body(j, carry):
                y = start_row + j
                found = plane_back(j)
                mask, shift = lines(see, y), lines(noi, y) - SHIFT
                values = tuple(
                    (mask * t + shift * plane(old, y, k)) * (1.0 / SCALE)
                    for k, t in enumerate(found)
                )
                store(new, y, values)
                first_stage(j, *values)
                return carry

            lax.fori_loop(0, count, body, 0, unroll=YU)
            emit(number + 1, slot, group)
            start(zcopies(which, slot, *group, new, target))

    def turn(c):
        for load in naturals[c]:
            load.wait()
        rows_of = pl.ds(c * chunk, chunk)

        def body(k, carry):
            deep = pl.ds(pl.multiple_of(k * tile, tile), tile)
            mask = jnp.swapaxes(snat[deep, rows_of], 0, 1).astype(F32)
            sown[rows_of, deep] = mask
            nown[rows_of, deep] = jnp.swapaxes(nnat[deep, rows_of], 0, 1)
            for i in range(columns):
                values = jnp.swapaxes(nat[i, deep, rows_of], 0, 1)
                p0[i // 2, rows_of, i % 2, deep] = values
                if odd:
                    wa[i, rows_of, 0, deep] = values * mask
                    wa[i, rows_of, 1, deep] = jnp.zeros_like(values)
                else:
                    wa[i // 2, rows_of, i % 2, deep] = values * mask
            return carry

        lax.fori_loop(0, depths, body, 0)

    pieces = ys // piece
    early = max(pieces - 1, 1)
    hop(0, 0)
    for c in range(chunks):
        turn(c)
        for k in range(c * chunk // piece, (c + 1) * chunk // piece):
            if k < early:
                start(zcopies(0, k, k * piece, piece, wa, w0))
    own_loads = [
        brought(0, spectrum, eig.at[slab.me]), brought(1, nown, noi.at[slab.me]),
        brought(2, sown, see.at[slab.me]),
    ]
    start(own_loads)
    relay(0)
    for k in range(early, pieces):
        start(zcopies(0, k, k * piece, piece, wa, w0))
    for load in loads:
        load.wait()
    for slot, (row, count) in enumerate(enter_groups):
        for k in range(row // piece, (row + count) // piece):
            finish(zcopies(0, k, k * piece, piece, wa, w0))

            def enter(j, carry):
                y = k * piece + j
                first_stage(y - row, plane(w0, y, 0), plane(w0, y, 1))
                return carry

            lax.fori_loop(0, piece, enter, 0, unroll=YU)
        if slot == max(len(enter_groups) - 2, 0):
            relay(0)
            for number in of_rows(0):
                hop(number, 0)
        emit(0, slot, (row, count))
    complete(0)
    relay(*of_rows(0))
    for c in range(1, chunks):
        for number in of_rows(c):
            hop(number, 0)
    finish(own_loads)
    xfinish(0, [by_rows(group) for group in enter_groups])
    middle(0)
    for c in range(chunks):
        relay(*of_rows(c))
    for c in range(1, chunks):
        relay(*of_rows(c))
    xfinish(1, [by_part(b) for b in range(blocks)])
    advance(1, w0, wa, x1, 1, lambda c: complete(*of_rows(c)))
    xfinish(2, [by_rows(group) for group in groups])
    middle(2)
    xfinish(3, [by_part(b) for b in range(blocks)])
    advance(3, wa, w0, x2, 2)
    xfinish(4, [by_rows(group) for group in groups])
    middle(4)
    for slot, group in enumerate(groups):
        finish(zcopies(1, slot, *group, wa, x1))
    xfinish(5, [by_part(b) for b in range(blocks)])
    for slot, group in enumerate(groups):
        absorb(5, group)

        def leave(j, carry):
            store(wa, group[0] + j, plane_back(j))
            return carry

        lax.fori_loop(0, group[1], leave, 0, unroll=YU)
        start(zcopies(3, slot, *group, wa, x3))

    def tiles(step, row):
        y = row + step // depths
        return y, pl.ds(pl.multiple_of(step % depths * tile, tile), tile)

    pairs = [(i, j) for i in range(columns) for j in range(i, columns)]
    zero = tuple(jnp.zeros((tile, nx), F32) for _ in pairs)
    lane = lax.broadcasted_iota(jnp.int32, stat.shape, 1)

    def at(ref, i, y, z):
        return ref[i, y, 0, z] if odd else ref[i // 2, y, i % 2, z]

    def base(ref, i, y, z):
        return ref[i // 2, y, i % 2, z]

    def note(moment, sums):
        for total, (i, j) in zip(sums, pairs):
            row = jnp.sum(total, axis=0, keepdims=True)
            rows[pl.ds(i * columns + j, 1)] = row
            if i != j:
                rows[pl.ds(j * columns + i, 1)] = row
        found = stat[...]
        for i in range(columns):
            column = jnp.sum(rows[pl.ds(i * columns, columns)], axis=1, keepdims=True)
            found = jnp.where(lane == moment * columns + i, column, found)
        stat[...] = found

    def moment(number, left_of, right_of):
        def body(step, sums):
            y, z = tiles(step, 0)
            lefts = [left_of(i, y, z) for i in range(columns)]
            rights = lefts if right_of is left_of else [right_of(i, y, z) for i in range(columns)]
            return tuple(s + lefts[i] * rights[j] for s, (i, j) in zip(sums, pairs))

        note(number, lax.fori_loop(0, ys * depths, body, zero))

    stat[...] = jnp.zeros(stat.shape, F32)
    for slot, group in enumerate(groups):
        finish(zcopies(2, slot, *group, w0, x2))

    def shape_basis(step, carry):
        y, z = tiles(step, 0)
        mask = sown[y, z] > 0
        factor = (nown[y, z] - SHIFT) * (1.0 / SCALE)
        for i in range(columns):
            once = factor * base(p0, i, y, z)
            place = (i, y, 0, z) if odd else (i // 2, y, i % 2, z)
            x1[place] = jnp.where(mask, x1[place], once)
            x2[place] = jnp.where(mask, x2[place], factor * once)
        return carry

    lax.fori_loop(0, ys * depths, shape_basis, 0)
    outs = [pltpu.make_async_copy(x1, p1_o, lsem.at[0]), pltpu.make_async_copy(x2, p2_o, lsem.at[1])]
    start(outs)
    of0, of1, of2 = (functools.partial(f, r) for f, r in ((base, p0), (at, x1), (at, x2)))
    for number, (l, r) in enumerate(((of0, of0), (of0, of1), (of1, of1), (of1, of2), (of2, of2))):
        moment(number, l, r)
    sums = zero
    for slot, group in enumerate(groups):
        finish(zcopies(3, slot, *group, wa, x3))

        def last(step, sums):
            y, z = tiles(step, group[0])
            mask = sown[y, z] * (1.0 / SCALE)
            factor = (nown[y, z] - SHIFT) * (1.0 / SCALE)
            lefts, rights = [], []
            for i in range(columns):
                place = (i, y, 0, z) if odd else (i // 2, y, i % 2, z)
                lefts.append(x2[place])
                rights.append(mask * x3[place] + factor * lefts[-1])
                x3[place] = rights[-1]
            return tuple(s + lefts[i] * rights[j] for s, (i, j) in zip(sums, pairs))

        sums = lax.fori_loop(0, group[1] * depths, last, sums)
    note(5, sums)
    out = pltpu.make_async_copy(x3, u2_o, lsem.at[2])
    out.start()
    for number in range(len(gathers)):
        for stage in range(slabs - 1):
            left(number, stage)
    part_sum[...] = spread(pencil, stat, one, s1, r1)
    found = spread(slab, part_sum, two, s2, r2)
    hankel = jnp.concatenate(
        [found[:, j * columns : (j + ITERS + 1) * columns] for j in range(ITERS + 1)], axis=0)
    c_ref[...], ok_ref[...] = small(hankel)
    finish(outs)
    out.wait()


def krylov(right, spectrum, noise, seen, tables):
    sizes = {name: lax.axis_size(name) for name in ("slab", "pencil")}
    slabs, pencils = sizes["slab"], sizes["pencil"]
    columns, depth, ys, nx = right.shape
    quads = columns // 2
    part, below, nz = spectrum.shape
    wide = 2 * nz
    chunk = 8 if ys % 8 == 0 else ys
    block = min(4, part)
    piece = min(4, chunk)
    planes = (slabs, ys, 2, depth, nx)
    gathered = (slabs, ys, depth, nx)
    sent = (pencils, part, ys, wide)
    groups = [(row, chunk) for row in range(0, ys, chunk)]
    enter_groups = groups[:-1] + [
        (row, piece) for row in range(groups[-1][0], ys, piece)
    ]
    slots = max(len(enter_groups), len(groups), part // block)
    chunks = ys // chunk
    any_space = pl.BlockSpec(memory_space=pl.ANY)
    vmem = pl.BlockSpec(memory_space=pltpu.VMEM)
    dma = pltpu.SemaphoreType.DMA
    tile = (columns, 128)
    scratch = (
        [pltpu.VMEM(planes, F32)] * 5
        + [pltpu.VMEM((slabs,) + spectrum.shape, F32)]
        + [pltpu.VMEM(gathered, F32)] * 2
        + [[pltpu.VMEM(sent, F32)] * 2, [pltpu.VMEM(sent, F32)] * 6]
        + [pltpu.VMEM((chunk, pencils, part, wide), F32)]
        + [pltpu.VMEM((quads, ys, 2, depth, nx), F32)]
        + [pltpu.VMEM((ys, depth, nx), F32)] * 2
        + [pltpu.VMEM(v.shape, v.dtype) for v in (right, noise, seen)]
        + [pltpu.VMEM(t.shape, BF16) for t in tables]
        + [pltpu.VMEM((columns * columns, nx), F32), pltpu.VMEM(tile, F32)]
        + total_scratch(sizes, tile)[:3]
        + [dma((6, slots, pencils))] * 2 + [dma((6, slots))]
        + [dma((4, ys // piece, slabs))] * 2 + [dma((4, ys // piece))]
        + [dma((1 + 2 * chunks, slabs, 2))] * 2 + [dma((4 * chunks + 6,))]
        + total_scratch(sizes, tile)[3:]
    )
    return pl.pallas_call(
        functools.partial(krylov_kernel, sizes, (
            chunk, block, piece, slabs == columns, enter_groups, groups)),
        in_specs=[any_space] * 10,
        out_specs=(any_space, any_space, any_space, vmem, vmem),
        out_shape=(jax.ShapeDtypeStruct(planes, F32),) * 3 + (
            jax.ShapeDtypeStruct(((ITERS + 1) * columns, columns), F32),
            jax.ShapeDtypeStruct((1, columns), F32),
        ),
        scratch_shapes=scratch,
        cost_estimate=pl.CostEstimate(flops=2**33, bytes_accessed=2**26, transcendentals=0),
        compiler_params=pltpu.CompilerParams(
            collective_id=0, has_side_effects=True, vmem_limit_bytes=60 * 2**20
        ),
    )(right, spectrum, noise, seen, *tables)


def recurrences(p0, p1, p2, u2):
    flat = lambda v: jnp.swapaxes(v, 1, 2).reshape(v.shape[0] * v.shape[2], -1)
    basis = [flat(v) for v in (p0, p1, p2, u2)]
    columns = basis[0].shape[0]

    def field(c):
        return sum(dot(c[k].T, basis[k]) for k in range(len(c)))

    def gram(u, v):
        return total_of(jnp.dot(u, v.T, precision=precise))

    def operator(c):
        zero = jnp.zeros((1, columns, columns), F32)
        return SHIFT * jnp.concatenate((c, zero)) + SCALE * jnp.concatenate((zero, c))

    def longer(c):
        return jnp.concatenate((c, jnp.zeros((1, columns, columns), F32)))

    residual = direction = answer = jnp.eye(columns, dtype=F32)[None]
    answer = 0.0 * answer
    vector = field(residual)
    gamma = gram(vector, vector)
    for iteration in range(ITERS):
        image = operator(direction)
        alpha = solve(gram(field(direction), field(image)), gamma)
        answer = answer + jnp.einsum("kij,jp->kip", direction, alpha, precision=precise)
        if iteration + 1 < ITERS:
            residual = longer(residual) - jnp.einsum("kij,jp->kip", image, alpha, precision=precise)
            vector = field(residual)
            gamma_next = gram(vector, vector)
            beta = solve(gamma, gamma_next)
            direction = residual + longer(
                jnp.einsum("kij,jp->kip", direction, beta, precision=precise)
            )
            answer = longer(answer)
            gamma = gamma_next
    return answer.reshape(-1, columns)


def local(right_sides, spectrum, noise_var, observed):
    columns, depth, ys, nx = right_sides.shape
    slabs, pencils = lax.axis_size("slab"), lax.axis_size("pencil")
    nz, ny = depth * slabs, ys * pencils
    quads = columns // 2
    odd = slabs == columns

    fx, gx = halves(embed(nx, True)), halves(embed(nx, False).T)
    fz, gz = halves(embed(nz, True).T), halves(embed(nz, False).T)
    fy, gy = halves(embed(ny, True)), halves(embed(ny, False, 1.0 / (nx * ny * nz)))
    tables = [jnp.asarray(t) for t in (fx, fz, gx, gz, fy, gy)]
    p1, p2, u2, coefficients, fine = krylov(right_sides, spectrum, noise_var, observed, tables)

    def slow():
        field = jnp.transpose(right_sides.reshape(quads, 2, depth, ys, nx), (0, 3, 1, 2, 4))
        basis = (p1, p2, u2)
        if odd:
            basis = [
                jnp.swapaxes(v[:, :, 0].reshape(quads, 2, ys, depth, nx), 1, 2) for v in basis
            ]
        return recurrences(field, *basis)

    coefficients = lax.cond(
        jnp.min(fine) > 0.5, lambda: coefficients[: 3 * columns], slow
    )
    tile = min(8, depth)
    planes = pl.BlockSpec(p1.shape[:3] + (tile, nx), lambda i: (0, 0, 0, i, 0))
    natural = pl.BlockSpec((columns, tile, ys, nx), lambda i: (0, i, 0, 0))
    return tuple(pl.pallas_call(
        functools.partial(final_kernel, odd),
        grid=(depth // tile,),
        in_specs=[pl.BlockSpec(memory_space=pltpu.SMEM), natural, planes, planes],
        out_specs=(natural, pl.BlockSpec((tile, ys, nx), lambda i: (i, 0, 0))),
        out_shape=(
            jax.ShapeDtypeStruct(right_sides.shape, F32),
            jax.ShapeDtypeStruct((depth, ys, nx), F32),
        ),
    )(coefficients, right_sides, p1, p2))


def solution(mesh):
    in_specs = (
        P(None, "slab", "pencil", None),
        P("pencil", "slab", None),
        P("slab", "pencil", None),
        P("slab", "pencil", None),
    )
    out_specs = (P(None, "slab", "pencil", None), P("slab", "pencil", None))
    return jax.shard_map(local, mesh=mesh, in_specs=in_specs, out_specs=out_specs, check_vma=False)
```

```python
import functools

import jax
import jax.numpy as jnp
import numpy as np
from jax import lax
from jax.experimental import pallas as pl
from jax.experimental.pallas import tpu as pltpu
from jax.sharding import PartitionSpec as P

ITERS = 3
SHIFT = 8.0
SCALE = 8.0
FLOOR = 1e-2
F32 = jnp.float32
BF16 = jnp.bfloat16

precise = lax.Precision.HIGHEST


def embed(length, forward, scale=1.0):
    points = np.arange(length)
    angles = (points[:, None] * points[None, :] % length) * (2.0 * np.pi / length)
    cosine, sine = np.cos(angles) * scale, np.sin(angles) * scale
    if not forward:
        sine = -sine
    return np.block([[cosine, sine], [-sine, cosine]])


def halves(table):
    table = np.asarray(table, np.float32)
    high = table.astype(BF16)
    low = (table - high.astype(np.float32)).astype(BF16)
    return np.stack((high, low))


def split(values):
    high = values.astype(BF16)
    return high, (values - high.astype(F32)).astype(BF16)


def dot3(left, right, dims=((1,), (0,))):
    mul = functools.partial(
        lax.dot_general, dimension_numbers=(dims, ((), ())), preferred_element_type=F32
    )
    return mul(left[0], right[0]) + (mul(left[1], right[0]) + mul(left[0], right[1]))


def solve(matrix, right_hand):
    size = matrix.shape[0]
    both = jnp.concatenate((0.5 * (matrix + matrix.T), right_hand), axis=1)
    place = lax.broadcasted_iota(jnp.int32, both.shape, 0)
    for i in range(size):
        row = both[i : i + 1] / both[i : i + 1, i : i + 1]
        both = jnp.where(place == i, row, both - both[:, i : i + 1] * row)
    return both[:, size:]


def small(moments, columns):
    span = ITERS * columns
    pick = lambda first, count: moments[:, first * columns : first * columns + count]
    both = jnp.concatenate([
        jnp.concatenate((SHIFT * pick(j, span) + SCALE * pick(j + 1, span), pick(j, columns)), axis=1)
        for j in range(ITERS)
    ], axis=0)
    place = lax.broadcasted_iota(jnp.int32, both.shape, 0)
    fine = jnp.ones((1, columns), F32)
    old = both
    for i in range(span):
        pivot = both[i : i + 1, i : i + 1]
        fine = jnp.where(pivot > FLOOR * old[i : i + 1, i : i + 1], fine, 0.0)
        row = both[i : i + 1] / pivot
        both = jnp.where(place == i, row, both - both[:, i : i + 1] * row)
    return both[:, span:], fine


def final_kernel(odd, c_ref, right, p1, p2, x_ref, g_ref):
    columns, tile, ys, _ = right.shape
    chunk = 8 if ys % 8 == 0 else ys

    def at(ref, i, y):
        return ref[i, pl.ds(y, chunk), 0] if odd else ref[i // 2, pl.ds(y, chunk), i % 2]

    for y in range(0, ys, chunk):
        rows = pl.ds(y, chunk)

        def column(p):
            found = 0.0
            for k, ref in ((1, p1), (2, p2)):
                for i in range(columns):
                    found = found + at(ref, i, y) * c_ref[k * columns + i, p]
            found = jnp.swapaxes(found, 0, 1)
            for i in range(columns):
                found = found + right[i, :, rows] * c_ref[i, p]
            x_ref[p, :, rows] = found
            return found

        def body(p, grad):
            return grad - right[p, :, rows] * column(p) * (0.5 / (columns - 1))

        first = column(0)
        g_ref[:, rows] = lax.fori_loop(1, columns, body, 0.5 * first * first)


QU, YU = 4, 4
MESH = pl.DeviceIdType.MESH


class Group:
    def __init__(self, sizes, axis):
        self.axis, self.size = axis, sizes[axis]
        self.names = tuple(sizes)
        self.place = {name: lax.axis_index(name) for name in sizes}
        self.me = self.place[axis]

    def peer(self, step):
        return lax.rem(self.me + step, self.size)

    def device(self, other):
        return tuple(other if name == self.axis else self.place[name] for name in self.names)

    def copy(self, src, dst, send, recv, other):
        return pltpu.make_async_remote_copy(
            src_ref=src, dst_ref=dst, send_sem=send, recv_sem=recv,
            device_id=self.device(other), device_id_type=MESH,
        )


def greet(groups):
    barrier = pltpu.get_barrier_semaphore()
    total = 0
    for group in groups:
        for step in range(1, group.size):
            pl.semaphore_signal(
                barrier, inc=1, device_id=group.device(group.peer(step)), device_id_type=MESH
            )
            total += 1
    return lambda: pl.semaphore_wait(barrier, total)


def spread(group, source, target, send, recv):
    copies = []
    for step in range(1, group.size):
        copy = group.copy(
            source, target.at[group.me], send.at[step], recv.at[step], group.peer(step)
        )
        copy.start()
        copies.append(copy)
    target[group.me] = source[...]
    for copy in copies:
        copy.wait()
    total = target[0]
    for place in range(1, group.size):
        total = total + target[place]
    return total


def total_kernel(sizes, v_ref, o_ref, part, one, two, send, recv, send2, recv2):
    slab, pencil = Group(sizes, "slab"), Group(sizes, "pencil")
    greet((slab, pencil))()
    part[...] = spread(pencil, v_ref, one, send, recv)
    o_ref[...] = spread(slab, part, two, send2, recv2)


def total_scratch(sizes, shape):
    return [
        pltpu.VMEM(shape, F32),
        pltpu.VMEM((sizes["pencil"],) + shape, F32),
        pltpu.VMEM((sizes["slab"],) + shape, F32),
        pltpu.SemaphoreType.DMA((sizes["pencil"],)),
        pltpu.SemaphoreType.DMA((sizes["pencil"],)),
        pltpu.SemaphoreType.DMA((sizes["slab"],)),
        pltpu.SemaphoreType.DMA((sizes["slab"],)),
    ]


def total_of(matrix):
    sizes = {name: lax.axis_size(name) for name in ("slab", "pencil")}
    rows, columns = matrix.shape
    wide = jnp.pad(matrix, ((0, 0), (0, 128 - columns)))
    found = pl.pallas_call(
        functools.partial(total_kernel, sizes),
        in_specs=[pl.BlockSpec(memory_space=pltpu.VMEM)],
        out_specs=pl.BlockSpec(memory_space=pltpu.VMEM),
        out_shape=jax.ShapeDtypeStruct(wide.shape, F32),
        scratch_shapes=total_scratch(sizes, wide.shape),
        compiler_params=pltpu.CompilerParams(collective_id=1, has_side_effects=True),
    )(wide)
    return found[:, :columns]


def krylov_kernel(
    sizes, plan,
    right, spectrum, noise, seen, fx_h, fz_h, gx_h, gz_h, fy_h, gy_h,
    p1_o, p2_o, u2_o, c_ref, ok_ref,
    w0, wa, x1, x2, x3, eig, noi, see, put, got, tmp, p0, nown, sown, nat, nnat, snat,
    fx, fz, gx, gz, fy, gy, rows, stat, part_sum, one, two,
    xsend, xrecv, xown, zsend, zrecv, zown, hsend, hrecv, lsem, s1, r1, s2, r2,
):
    slab, pencil = Group(sizes, "slab"), Group(sizes, "pencil")
    slabs, pencils = slab.size, pencil.size
    _, ys, _, depth, nx = w0.shape
    part, wide = got[0].shape[1], got[0].shape[3]
    nz = wide // 2
    chunk, block, piece, odd, enter_groups, groups = plan
    chunks, blocks = ys // chunk, part // block
    columns = right.shape[0]
    tile = min(8, depth)
    depths = depth // tile

    def brought(slot, src, dst):
        return pltpu.make_async_copy(src, dst, lsem.at[slot])

    met = greet((slab, pencil))
    naturals = []
    for c in range(chunks):
        span = pl.ds(c * chunk, chunk)
        naturals.append([
            brought(4 * c, seen.at[:, span], snat.at[:, span]),
            brought(4 * c + 1, right.at[:, :, span], nat.at[:, :, span]),
            brought(4 * c + 2, noise.at[:, span], nnat.at[:, span]),
        ])
        for load in naturals[-1]:
            load.start()
    tables = ((fx_h, fx), (fz_h, fz), (gx_h, gx), (gz_h, gz), (fy_h, fy), (gy_h, gy))
    loads = [brought(4 * chunks + i, a, b) for i, (a, b) in enumerate(tables)]
    for load in loads:
        load.start()

    def zrows(ref, y, count):
        return ref.at[:, pl.ds(y, count)]

    def zcopies(number, slot, y, count, src, dst):
        made = []
        for step in range(1, slabs):
            other = slab.peer(step)
            made.append(slab.copy(
                src.at[other, pl.ds(y, count)], dst.at[slab.me, pl.ds(y, count)],
                zsend.at[number, slot, step], zrecv.at[number, slot, step], other,
            ))
        made.append(pltpu.make_async_copy(
            src.at[slab.me, pl.ds(y, count)], dst.at[slab.me, pl.ds(y, count)],
            zown.at[number, slot],
        ))
        return made

    def start(copies):
        for copy in copies:
            copy.start()

    def finish(copies):
        for copy in copies:
            copy.wait()

    gathers = [(spectrum, lambda place: eig.at[place])]
    for c in range(chunks):
        span = pl.ds(c * chunk, chunk)
        for own, full in ((nown, noi), (sown, see)):
            gathers.append((
                own.at[span],
                functools.partial(lambda full, span, place: full.at[place, span], full, span),
            ))
    stages = [0] * len(gathers)

    def hop(number, stage):
        own, full = gathers[number]
        sems = lambda way: (hsend.at[number, stage, way], hrecv.at[number, stage, way])

        def send(way, origin, other):
            src = own if stage == 0 else full(origin)
            slab.copy(src, full(origin), *sems(way), other).start()

        @pl.when((slab.me + 1 < slabs) & (slab.me >= stage))
        def _():
            send(0, slab.me - stage, slab.me + 1)

        @pl.when((slab.me >= 1) & (slab.me + stage < slabs))
        def _():
            send(1, slab.me + stage, slab.me - 1)

    def halted(number, stage, way):
        own, full = gathers[number]
        return slab.copy(
            own, full(slab.me), hsend.at[number, stage, way], hrecv.at[number, stage, way],
            slab.peer(1),
        )

    def landed(number, stage):
        @pl.when(slab.me >= 1 + stage)
        def _():
            halted(number, stage, 0).wait_recv()

        @pl.when(slab.me + 1 + stage < slabs)
        def _():
            halted(number, stage, 1).wait_recv()

    def left(number, stage):
        @pl.when((slab.me + 1 < slabs) & (slab.me >= stage))
        def _():
            halted(number, stage, 0).wait_send()

        @pl.when((slab.me >= 1) & (slab.me + stage < slabs))
        def _():
            halted(number, stage, 1).wait_send()

    def relay(*numbers):
        for number in numbers:
            stage = stages[number]
            if stage + 1 < slabs:
                landed(number, stage)
                if stage + 2 < slabs:
                    hop(number, stage + 1)
                stages[number] = stage + 1

    def complete(*numbers):
        for _ in range(slabs - 1):
            relay(*numbers)

    def of_rows(c):
        return (1 + 2 * c, 2 + 2 * c)

    def xcopy(number, slot, step, view):
        other = pencil.peer(step)
        return pencil.copy(
            view(put[number % 2], other), view(got[number], pencil.me),
            xsend.at[number, slot, step], xrecv.at[number, slot, step], other,
        )

    def xself(number, slot, view):
        return pltpu.make_async_copy(
            view(put[number % 2], pencil.me), view(got[number], pencil.me), xown.at[number, slot]
        )

    def by_rows(group):
        return lambda ref, place: ref.at[place, :, pl.ds(*group)]

    def by_part(b):
        return lambda ref, place: ref.at[place, pl.ds(b * block, block)]

    def xfinish(number, views):
        for slot, view in enumerate(views):
            for step in range(1, pencils):
                xcopy(number, slot, step, view).wait()
            xself(number, slot, view).wait()

    def first_stage(j, real, imag):
        length = real.shape[1]
        data = split(jnp.concatenate((real, imag), axis=1))
        first = dot3((fx[0], fx[1]), data, ((1,), (1,)))
        first = jnp.concatenate((first[:length], first[length:]), axis=1)
        for q in range(pencils):
            tmp[j, q] = first[q * part : (q + 1) * part]

    def emit(number, slot, group):
        span, count = pl.ds(*group), group[1]

        def one_block(q):
            data = jnp.concatenate([tmp[j, q] for j in range(count)], axis=0)
            out = dot3(split(data), (fz[0], fz[1]))
            out = jnp.stack([out[j * part : (j + 1) * part] for j in range(count)])
            put[number % 2][q, :, span] = jnp.swapaxes(out, 0, 1)

        def body(step, carry):
            one_block(pencil.peer(step))
            xcopy(number, slot, step, by_rows(group)).start()
            return carry

        lax.fori_loop(1, pencils, body, 0, unroll=QU)
        one_block(pencil.me)
        xself(number, slot, by_rows(group)).start()

    def absorb(number, group):
        span, count = pl.ds(*group), group[1]

        def body(q, carry):
            data = jnp.swapaxes(got[number][q, :, span], 0, 1)
            data = jnp.concatenate([data[j] for j in range(count)], axis=0)
            out = dot3(split(data), (gz[0], gz[1]))
            for j in range(count):
                tmp[j, q] = out[j * part : (j + 1) * part]
            return carry

        lax.fori_loop(0, pencils, body, 0, unroll=QU)

    def plane_back(j):
        first = jnp.concatenate([tmp[j, q] for q in range(pencils)], axis=0)
        first = jnp.concatenate((first[:, :nz], first[:, nz:]), axis=0)
        plane = dot3(split(first), (gx[0], gx[1]), ((0,), (0,)))
        return plane[:, :nx], plane[:, nx:]

    def lines(ref, y):
        return jnp.concatenate([ref[s, y] for s in range(slabs)], axis=0)

    def plane(ref, y, c):
        return jnp.concatenate([ref[s, y, c] for s in range(slabs)], axis=0)

    def store(ref, y, values):
        for c in range(2):
            for s in range(slabs):
                ref[s, y, c] = values[c][s * depth : (s + 1) * depth]

    def middle(number, after=None):
        def body(b, carry):
            for a2 in range(0, block, 2):
                spots = range(a2, min(a2 + 2, block))
                halves_of = []
                for a in spots:
                    data = jnp.concatenate(
                        [got[number][q, b * block + a] for q in range(pencils)], axis=0)
                    halves_of.append(jnp.concatenate((data[:, :nz], data[:, nz:]), axis=0))
                spec = dot3((fy[0], fy[1]), split(jnp.concatenate(halves_of, axis=1)))
                eigen = jnp.concatenate([
                    jnp.concatenate([eig[s, b * block + a] for s in range(slabs)], axis=0)
                    for a in spots], axis=1)
                spec = spec * jnp.concatenate((eigen, eigen), axis=0)
                back = dot3((gy[0], gy[1]), split(spec))
                ny = back.shape[0] // 2
                for k, a in enumerate(spots):
                    mine = back[:, k * nz : (k + 1) * nz]
                    mine = jnp.concatenate((mine[:ny], mine[ny:]), axis=1)
                    for q in range(pencils):
                        put[(number + 1) % 2][q, b * block + a] = mine[q * ys : (q + 1) * ys]
            for step in range(1, pencils):
                xcopy(number + 1, b, step, by_part(b)).start()
            xself(number + 1, b, by_part(b)).start()
            return carry

        lax.fori_loop(0, blocks, body, 0)

    def advance(number, old, new, target, which, ready=None):
        for slot, group in enumerate(groups):
            start_row, count = group
            absorb(number, group)
            if ready is not None:
                ready(start_row // chunk)

            def body(j, carry):
                y = start_row + j
                found = plane_back(j)
                mask, shift = lines(see, y), lines(noi, y) - SHIFT
                values = tuple(
                    (mask * t + shift * plane(old, y, k)) * (1.0 / SCALE)
                    for k, t in enumerate(found)
                )
                store(new, y, values)
                first_stage(j, *values)
                return carry

            lax.fori_loop(0, count, body, 0, unroll=YU)
            emit(number + 1, slot, group)
            start(zcopies(which, slot, *group, new, target))

    def turn(c):
        for load in naturals[c]:
            load.wait()
        rows_of = pl.ds(c * chunk, chunk)

        def body(k, carry):
            deep = pl.ds(pl.multiple_of(k * tile, tile), tile)
            mask = jnp.swapaxes(snat[deep, rows_of], 0, 1).astype(F32)
            sown[rows_of, deep] = mask
            nown[rows_of, deep] = jnp.swapaxes(nnat[deep, rows_of], 0, 1)
            for i in range(columns):
                values = jnp.swapaxes(nat[i, deep, rows_of], 0, 1)
                p0[i // 2, rows_of, i % 2, deep] = values
                if odd:
                    wa[i, rows_of, 0, deep] = values * mask
                    wa[i, rows_of, 1, deep] = jnp.zeros_like(values)
                else:
                    wa[i // 2, rows_of, i % 2, deep] = values * mask
            return carry

        lax.fori_loop(0, depths, body, 0)

    pieces = ys // piece
    early = max(pieces - 1, 1)
    for c in range(chunks):
        turn(c)
        if c == 0:
            met()
            hop(0, 0)
        for k in range(c * chunk // piece, (c + 1) * chunk // piece):
            if k < early:
                start(zcopies(0, k, k * piece, piece, wa, w0))
    own_loads = [
        brought(0, spectrum, eig.at[slab.me]), brought(1, nown, noi.at[slab.me]),
        brought(2, sown, see.at[slab.me]),
    ]
    start(own_loads)
    relay(0)
    for k in range(early, pieces):
        start(zcopies(0, k, k * piece, piece, wa, w0))
    for load in loads:
        load.wait()
    for slot, (row, count) in enumerate(enter_groups):
        for k in range(row // piece, (row + count) // piece):
            finish(zcopies(0, k, k * piece, piece, wa, w0))

            def enter(j, carry):
                y = k * piece + j
                first_stage(y - row, plane(w0, y, 0), plane(w0, y, 1))
                return carry

            lax.fori_loop(0, piece, enter, 0, unroll=YU)
        if slot == max(len(enter_groups) - 2, 0):
            relay(0)
            for number in of_rows(0):
                hop(number, 0)
        emit(0, slot, (row, count))
    complete(0)
    relay(*of_rows(0))
    for c in range(1, chunks):
        for number in of_rows(c):
            hop(number, 0)
    finish(own_loads)
    xfinish(0, [by_rows(group) for group in enter_groups])
    middle(0)
    for c in range(chunks):
        relay(*of_rows(c))
    for c in range(1, chunks):
        relay(*of_rows(c))
    xfinish(1, [by_part(b) for b in range(blocks)])
    advance(1, w0, wa, x1, 1, lambda c: complete(*of_rows(c)))
    xfinish(2, [by_rows(group) for group in groups])
    middle(2)
    xfinish(3, [by_part(b) for b in range(blocks)])
    advance(3, wa, w0, x2, 2)
    xfinish(4, [by_rows(group) for group in groups])
    middle(4)
    for slot, group in enumerate(groups):
        finish(zcopies(1, slot, *group, wa, x1))
    xfinish(5, [by_part(b) for b in range(blocks)])
    for group in [(row, chunk) for row in range(0, ys, chunk)]:
        absorb(5, group)

        for row in range(group[0], sum(group), piece):
            def leave(j, carry):
                store(wa, row + j, plane_back(row - group[0] + j))
                return carry

            lax.fori_loop(0, piece, leave, 0, unroll=YU)
            start(zcopies(3, row // piece, row, piece, wa, x3))

    def tiles(step, row):
        y = row + step // depths
        return y, pl.ds(pl.multiple_of(step % depths * tile, tile), tile)

    pairs = [(i, j) for i in range(columns) for j in range(i, columns)]
    zero = tuple(jnp.zeros((tile, nx), F32) for _ in pairs)
    lane = lax.broadcasted_iota(jnp.int32, stat.shape, 1)

    def at(ref, i, y, z):
        return ref[i, y, 0, z] if odd else ref[i // 2, y, i % 2, z]

    def base(ref, i, y, z):
        return ref[i // 2, y, i % 2, z]

    def note(moment, sums):
        for total, (i, j) in zip(sums, pairs):
            row = jnp.sum(total, axis=0, keepdims=True)
            rows[pl.ds(i * columns + j, 1)] = row
            if i != j:
                rows[pl.ds(j * columns + i, 1)] = row
        found = stat[...]
        for i in range(columns):
            column = jnp.sum(rows[pl.ds(i * columns, columns)], axis=1, keepdims=True)
            found = jnp.where(lane == moment * columns + i, column, found)
        stat[...] = found

    def moment(number, left_of, right_of):
        def body(step, sums):
            y, z = tiles(step, 0)
            lefts = [left_of(i, y, z) for i in range(columns)]
            rights = lefts if right_of is left_of else [right_of(i, y, z) for i in range(columns)]
            return tuple(s + lefts[i] * rights[j] for s, (i, j) in zip(sums, pairs))

        note(number, lax.fori_loop(0, ys * depths, body, zero))

    stat[...] = jnp.zeros(stat.shape, F32)
    for slot, group in enumerate(groups):
        finish(zcopies(2, slot, *group, w0, x2))

    def shape_basis(step, carry):
        y, z = tiles(step, 0)
        mask = sown[y, z] > 0
        factor = (nown[y, z] - SHIFT) * (1.0 / SCALE)
        for i in range(columns):
            once = factor * base(p0, i, y, z)
            place = (i, y, 0, z) if odd else (i // 2, y, i % 2, z)
            x1[place] = jnp.where(mask, x1[place], once)
            x2[place] = jnp.where(mask, x2[place], factor * once)
        return carry

    lax.fori_loop(0, ys * depths, shape_basis, 0)
    outs = [pltpu.make_async_copy(x1, p1_o, lsem.at[0]), pltpu.make_async_copy(x2, p2_o, lsem.at[1])]
    start(outs)
    of0, of1, of2 = (functools.partial(f, r) for f, r in ((base, p0), (at, x1), (at, x2)))
    for number, (l, r) in enumerate(((of0, of0), (of0, of1), (of1, of1), (of1, of2), (of2, of2))):
        moment(number, l, r)
    sums = zero
    for k in range(pieces):
        finish(zcopies(3, k, k * piece, piece, wa, x3))

        def last(step, sums):
            y, z = tiles(step, k * piece)
            mask = sown[y, z] * (1.0 / SCALE)
            factor = (nown[y, z] - SHIFT) * (1.0 / SCALE)
            lefts, rights = [], []
            for i in range(columns):
                place = (i, y, 0, z) if odd else (i // 2, y, i % 2, z)
                lefts.append(x2[place])
                rights.append(mask * x3[place] + factor * lefts[-1])
                x3[place] = rights[-1]
            return tuple(s + lefts[i] * rights[j] for s, (i, j) in zip(sums, pairs))

        sums = lax.fori_loop(0, piece * depths, last, sums)
    note(5, sums)
    out = pltpu.make_async_copy(x3, u2_o, lsem.at[2])
    out.start()
    for number in range(len(gathers)):
        for stage in range(slabs - 1):
            left(number, stage)
    part_sum[...] = spread(pencil, stat, one, s1, r1)
    found = spread(slab, part_sum, two, s2, r2)
    c_ref[...], ok_ref[...] = small(found, columns)
    finish(outs)
    out.wait()


def krylov(right, spectrum, noise, seen, tables):
    sizes = {name: lax.axis_size(name) for name in ("slab", "pencil")}
    slabs, pencils = sizes["slab"], sizes["pencil"]
    columns, depth, ys, nx = right.shape
    quads = columns // 2
    part, below, nz = spectrum.shape
    wide = 2 * nz
    chunk = 8 if ys % 8 == 0 else ys
    block = min(4, part)
    piece = min(4, chunk)
    planes = (slabs, ys, 2, depth, nx)
    gathered = (slabs, ys, depth, nx)
    sent = (pencils, part, ys, wide)
    whole_groups = [(row, chunk) for row in range(0, ys, chunk)]
    enter_groups = whole_groups[:-1] + [(row, piece) for row in range(ys - chunk, ys, piece)]
    groups = [(row, piece) for row in range(0, chunk, piece)] + whole_groups[1:]
    slots = max(len(enter_groups), len(groups), part // block)
    chunks = ys // chunk
    any_space = pl.BlockSpec(memory_space=pl.ANY)
    vmem = pl.BlockSpec(memory_space=pltpu.VMEM)
    dma = pltpu.SemaphoreType.DMA
    tile = (columns, 128)
    scratch = (
        [pltpu.VMEM(planes, F32)] * 5
        + [pltpu.VMEM((slabs,) + spectrum.shape, F32)]
        + [pltpu.VMEM(gathered, F32)] * 2
        + [[pltpu.VMEM(sent, F32)] * 2, [pltpu.VMEM(sent, F32)] * 6]
        + [pltpu.VMEM((chunk, pencils, part, wide), F32)]
        + [pltpu.VMEM((quads, ys, 2, depth, nx), F32)]
        + [pltpu.VMEM((ys, depth, nx), F32)] * 2
        + [pltpu.VMEM(v.shape, v.dtype) for v in (right, noise, seen)]
        + [pltpu.VMEM(t.shape, BF16) for t in tables]
        + [pltpu.VMEM((columns * columns, nx), F32), pltpu.VMEM(tile, F32)]
        + total_scratch(sizes, tile)[:3]
        + [dma((6, slots, pencils))] * 2 + [dma((6, slots))]
        + [dma((4, ys // piece, slabs))] * 2 + [dma((4, ys // piece))]
        + [dma((1 + 2 * chunks, slabs, 2))] * 2 + [dma((4 * chunks + 6,))]
        + total_scratch(sizes, tile)[3:]
    )
    return pl.pallas_call(
        functools.partial(krylov_kernel, sizes, (
            chunk, block, piece, slabs == columns, enter_groups, groups)),
        in_specs=[any_space] * 10,
        out_specs=(any_space, any_space, any_space, vmem, vmem),
        out_shape=(jax.ShapeDtypeStruct(planes, F32),) * 3 + (
            jax.ShapeDtypeStruct((ITERS * columns, columns), F32),
            jax.ShapeDtypeStruct((1, columns), F32),
        ),
        scratch_shapes=scratch,
        cost_estimate=pl.CostEstimate(flops=2**33, bytes_accessed=2**26, transcendentals=0),
        compiler_params=pltpu.CompilerParams(
            collective_id=0, has_side_effects=True, vmem_limit_bytes=60 * 2**20
        ),
    )(right, spectrum, noise, seen, *tables)


def mixed_kernel(odd, u_ref, v_ref, p0, p1, p2, p3, o_ref):
    quads, ys, _, depth, nx = p0.shape
    columns = 2 * quads
    tile = min(8, depth)
    pairs = [(i, j) for i in range(columns) for j in range(i, columns)]

    def body(step, sums):
        y, z = step // (depth // tile), pl.ds(pl.multiple_of(step % (depth // tile) * tile, tile), tile)
        tiles = [p0[i // 2, y, i % 2, z] for i in range(columns)]
        for ref in (p1, p2, p3):
            for i in range(columns):
                tiles.append(ref[i, y, 0, z] if odd else ref[i // 2, y, i % 2, z])
        left, right = (
            [sum(t * c_ref[k, i] for k, t in enumerate(tiles)) for i in range(columns)]
            for c_ref in (u_ref, v_ref)
        )
        return tuple(s + left[i] * right[j] for s, (i, j) in zip(sums, pairs))

    zero = jnp.zeros((tile, nx), F32)
    sums = lax.fori_loop(0, ys * (depth // tile), body, (zero,) * len(pairs))
    for total, (i, j) in zip(sums, pairs):
        row = jnp.sum(total, axis=0, keepdims=True)
        o_ref[pl.ds(i * columns + j, 1)] = row
        if i != j:
            o_ref[pl.ds(j * columns + i, 1)] = row


def recurrences(odd, basis):
    columns = 2 * basis[0].shape[0]

    def gram(u, v):
        wide = [
            jnp.pad(c.reshape(-1, columns), ((0, (ITERS + 1 - len(c)) * columns), (0, 0)))
            for c in (u, v)
        ]
        rows = pl.pallas_call(
            functools.partial(mixed_kernel, odd),
            in_specs=[pl.BlockSpec(memory_space=pltpu.SMEM)] * 2
            + [pl.BlockSpec(memory_space=pltpu.VMEM)] * 4,
            out_shape=jax.ShapeDtypeStruct((columns * columns, basis[0].shape[-1]), F32),
        )(*wide, *basis)
        return total_of(jnp.sum(rows, axis=1).reshape(columns, columns))

    def operator(c):
        zero = jnp.zeros((1, columns, columns), F32)
        return SHIFT * jnp.concatenate((c, zero)) + SCALE * jnp.concatenate((zero, c))

    def longer(c):
        return jnp.concatenate((c, jnp.zeros((1, columns, columns), F32)))

    residual = direction = answer = jnp.eye(columns, dtype=F32)[None]
    answer = 0.0 * answer
    gamma = gram(residual, residual)
    for iteration in range(ITERS):
        image = operator(direction)
        alpha = solve(gram(direction, image), gamma)
        answer = answer + jnp.einsum("kij,jp->kip", direction, alpha, precision=precise)
        if iteration + 1 < ITERS:
            residual = longer(residual) - jnp.einsum("kij,jp->kip", image, alpha, precision=precise)
            gamma_next = gram(residual, residual)
            beta = solve(gamma, gamma_next)
            direction = residual + longer(
                jnp.einsum("kij,jp->kip", direction, beta, precision=precise)
            )
            answer = longer(answer)
            gamma = gamma_next
    return answer.reshape(-1, columns)


def local(right_sides, spectrum, noise_var, observed):
    columns, depth, ys, nx = right_sides.shape
    slabs, pencils = lax.axis_size("slab"), lax.axis_size("pencil")
    nz, ny = depth * slabs, ys * pencils
    quads = columns // 2
    odd = slabs == columns

    fx, gx = halves(embed(nx, True)), halves(embed(nx, False).T)
    fz, gz = halves(embed(nz, True).T), halves(embed(nz, False).T)
    fy, gy = halves(embed(ny, True)), halves(embed(ny, False, 1.0 / (nx * ny * nz)))
    tables = [jnp.asarray(t) for t in (fx, fz, gx, gz, fy, gy)]
    p1, p2, u2, coefficients, fine = krylov(right_sides, spectrum, noise_var, observed, tables)

    def slow():
        field = jnp.transpose(right_sides.reshape(quads, 2, depth, ys, nx), (0, 3, 1, 2, 4))
        return recurrences(odd, (field, p1, p2, u2))

    coefficients = lax.cond(
        jnp.min(fine) > 0.5, lambda: coefficients, slow
    )
    tile = min(8, depth)
    planes = pl.BlockSpec(p1.shape[:3] + (tile, nx), lambda i: (0, 0, 0, i, 0))
    natural = pl.BlockSpec((columns, tile, ys, nx), lambda i: (0, i, 0, 0))
    return tuple(pl.pallas_call(
        functools.partial(final_kernel, odd),
        grid=(depth // tile,),
        in_specs=[pl.BlockSpec(memory_space=pltpu.SMEM), natural, planes, planes],
        out_specs=(natural, pl.BlockSpec((tile, ys, nx), lambda i: (i, 0, 0))),
        out_shape=(
            jax.ShapeDtypeStruct(right_sides.shape, F32),
            jax.ShapeDtypeStruct((depth, ys, nx), F32),
        ),
    )(coefficients, right_sides, p1, p2))


def solution(mesh):
    in_specs = (
        P(None, "slab", "pencil", None),
        P("pencil", "slab", None),
        P("slab", "pencil", None),
        P("slab", "pencil", None),
    )
    out_specs = (P(None, "slab", "pencil", None), P("slab", "pencil", None))
    return jax.shard_map(local, mesh=mesh, in_specs=in_specs, out_specs=out_specs, check_vma=False)
```

```python
import functools

import jax
import jax.numpy as jnp
import numpy as np
from jax import lax
from jax.experimental import pallas as pl
from jax.experimental.pallas import tpu as pltpu
from jax.sharding import PartitionSpec as P

ITERS = 3
SHIFT = 8.0
SCALE = 8.0
FLOOR = 1e-2
F32 = jnp.float32
BF16 = jnp.bfloat16

precise = lax.Precision.HIGHEST


def embed(length, forward, scale=1.0):
    points = np.arange(length)
    angles = (points[:, None] * points[None, :] % length) * (2.0 * np.pi / length)
    cosine, sine = np.cos(angles) * scale, np.sin(angles) * scale
    if not forward:
        sine = -sine
    return np.block([[cosine, sine], [-sine, cosine]])


def halves(table):
    table = np.asarray(table, np.float32)
    high = table.astype(BF16)
    low = (table - high.astype(np.float32)).astype(BF16)
    return np.stack((high, low))


def split(values):
    high = values.astype(BF16)
    return high, (values - high.astype(F32)).astype(BF16)


def dot3(left, right, dims=((1,), (0,))):
    mul = functools.partial(
        lax.dot_general, dimension_numbers=(dims, ((), ())), preferred_element_type=F32
    )
    return mul(left[0], right[0]) + (mul(left[1], right[0]) + mul(left[0], right[1]))


def solve(matrix, right_hand):
    size = matrix.shape[0]
    both = jnp.concatenate((0.5 * (matrix + matrix.T), right_hand), axis=1)
    place = lax.broadcasted_iota(jnp.int32, both.shape, 0)
    for i in range(size):
        row = both[i : i + 1] / both[i : i + 1, i : i + 1]
        both = jnp.where(place == i, row, both - both[:, i : i + 1] * row)
    return both[:, size:]


def small(moments, columns):
    span = ITERS * columns
    pick = lambda first, count: moments[:, first * columns : first * columns + count]
    both = jnp.concatenate([
        jnp.concatenate((SHIFT * pick(j, span) + SCALE * pick(j + 1, span), pick(j, columns)), axis=1)
        for j in range(ITERS)
    ], axis=0)
    place = lax.broadcasted_iota(jnp.int32, both.shape, 0)
    fine = jnp.ones((1, columns), F32)
    old = both
    for i in range(span):
        pivot = both[i : i + 1, i : i + 1]
        fine = jnp.where(pivot > FLOOR * old[i : i + 1, i : i + 1], fine, 0.0)
        row = both[i : i + 1] / pivot
        both = jnp.where(place == i, row, both - both[:, i : i + 1] * row)
    return both[:, span:], fine


def final_kernel(odd, c_ref, right, p1, p2, x_ref, g_ref):
    columns, tile, ys, _ = right.shape
    chunk = 8 if ys % 8 == 0 else ys

    def at(ref, i, y):
        return ref[i, pl.ds(y, chunk), 0] if odd else ref[i // 2, pl.ds(y, chunk), i % 2]

    for y in range(0, ys, chunk):
        rows = pl.ds(y, chunk)

        def column(p):
            found = 0.0
            for k, ref in ((1, p1), (2, p2)):
                for i in range(columns):
                    found = found + at(ref, i, y) * c_ref[k * columns + i, p]
            found = jnp.swapaxes(found, 0, 1)
            for i in range(columns):
                found = found + right[i, :, rows] * c_ref[i, p]
            x_ref[p, :, rows] = found
            return found

        def body(p, grad):
            return grad - right[p, :, rows] * column(p) * (0.5 / (columns - 1))

        first = column(0)
        g_ref[:, rows] = lax.fori_loop(1, columns, body, 0.5 * first * first)


QU, YU = 4, 4
MESH = pl.DeviceIdType.MESH


class Group:
    def __init__(self, sizes, axis):
        self.axis, self.size = axis, sizes[axis]
        self.names = tuple(sizes)
        self.place = {name: lax.axis_index(name) for name in sizes}
        self.me = self.place[axis]

    def peer(self, step):
        return lax.rem(self.me + step, self.size)

    def device(self, other):
        return tuple(other if name == self.axis else self.place[name] for name in self.names)

    def copy(self, src, dst, send, recv, other):
        return pltpu.make_async_remote_copy(
            src_ref=src, dst_ref=dst, send_sem=send, recv_sem=recv,
            device_id=self.device(other), device_id_type=MESH,
        )


def greet(groups):
    barrier = pltpu.get_barrier_semaphore()
    total = 0
    for group in groups:
        for step in range(1, group.size):
            pl.semaphore_signal(
                barrier, inc=1, device_id=group.device(group.peer(step)), device_id_type=MESH
            )
            total += 1
    return lambda: pl.semaphore_wait(barrier, total)


def spread(group, source, target, send, recv):
    copies = []
    for step in range(1, group.size):
        copy = group.copy(
            source, target.at[group.me], send.at[step], recv.at[step], group.peer(step)
        )
        copy.start()
        copies.append(copy)
    target[group.me] = source[...]
    for copy in copies:
        copy.wait()
    total = target[0]
    for place in range(1, group.size):
        total = total + target[place]
    return total


def total_kernel(sizes, v_ref, o_ref, part, one, two, send, recv, send2, recv2):
    slab, pencil = Group(sizes, "slab"), Group(sizes, "pencil")
    greet((slab, pencil))()
    part[...] = spread(pencil, v_ref, one, send, recv)
    o_ref[...] = spread(slab, part, two, send2, recv2)


def total_scratch(sizes, shape):
    return [
        pltpu.VMEM(shape, F32),
        pltpu.VMEM((sizes["pencil"],) + shape, F32),
        pltpu.VMEM((sizes["slab"],) + shape, F32),
        pltpu.SemaphoreType.DMA((sizes["pencil"],)),
        pltpu.SemaphoreType.DMA((sizes["pencil"],)),
        pltpu.SemaphoreType.DMA((sizes["slab"],)),
        pltpu.SemaphoreType.DMA((sizes["slab"],)),
    ]


def total_of(matrix):
    sizes = {name: lax.axis_size(name) for name in ("slab", "pencil")}
    rows, columns = matrix.shape
    wide = jnp.pad(matrix, ((0, 0), (0, 128 - columns)))
    found = pl.pallas_call(
        functools.partial(total_kernel, sizes),
        in_specs=[pl.BlockSpec(memory_space=pltpu.VMEM)],
        out_specs=pl.BlockSpec(memory_space=pltpu.VMEM),
        out_shape=jax.ShapeDtypeStruct(wide.shape, F32),
        scratch_shapes=total_scratch(sizes, wide.shape),
        compiler_params=pltpu.CompilerParams(collective_id=1, has_side_effects=True),
    )(wide)
    return found[:, :columns]


def krylov_kernel(
    sizes, plan,
    right, spectrum, noise, seen, fx_h, fz_h, gx_h, gz_h, fy_h, gy_h,
    p1_o, p2_o, u2_o, c_ref, ok_ref,
    w0, wa, x1, x2, x3, eig, noi, see, put, got, tmp, p0, nown, sown, nat, nnat, snat,
    fx, fz, gx, gz, fy, gy, rows, stat, part_sum, one, two,
    xsend, xrecv, xown, zsend, zrecv, zown, hsend, hrecv, lsem, s1, r1, s2, r2,
):
    slab, pencil = Group(sizes, "slab"), Group(sizes, "pencil")
    slabs, pencils = slab.size, pencil.size
    _, ys, _, depth, nx = w0.shape
    part, wide = got[0].shape[1], got[0].shape[3]
    nz = wide // 2
    chunk, block, piece, odd, enter_groups, groups = plan
    chunks, blocks = ys // chunk, part // block
    columns = right.shape[0]
    tile = min(8, depth)
    depths = depth // tile

    def brought(slot, src, dst):
        return pltpu.make_async_copy(src, dst, lsem.at[slot])

    met = greet((slab, pencil))
    naturals = []
    for c in range(chunks):
        span = pl.ds(c * chunk, chunk)
        naturals.append([
            brought(4 * c, seen.at[:, span], snat.at[:, span]),
            brought(4 * c + 1, right.at[:, :, span], nat.at[:, :, span]),
            brought(4 * c + 2, noise.at[:, span], nnat.at[:, span]),
        ])
        for load in naturals[-1]:
            load.start()
    tables = ((fx_h, fx), (fz_h, fz), (gx_h, gx), (gz_h, gz), (fy_h, fy), (gy_h, gy))
    loads = [brought(4 * chunks + i, a, b) for i, (a, b) in enumerate(tables)]
    for load in loads:
        load.start()

    def zrows(ref, y, count):
        return ref.at[:, pl.ds(y, count)]

    def zcopies(number, slot, y, count, src, dst):
        made = []
        for step in range(1, slabs):
            other = slab.peer(step)
            made.append(slab.copy(
                src.at[other, pl.ds(y, count)], dst.at[slab.me, pl.ds(y, count)],
                zsend.at[number, slot, step], zrecv.at[number, slot, step], other,
            ))
        made.append(pltpu.make_async_copy(
            src.at[slab.me, pl.ds(y, count)], dst.at[slab.me, pl.ds(y, count)],
            zown.at[number, slot],
        ))
        return made

    def start(copies):
        for copy in copies:
            copy.start()

    def finish(copies):
        for copy in copies:
            copy.wait()

    gathers = []
    for b in range(blocks):
        span = pl.ds(b * block, block)
        gathers.append((
            spectrum.at[span], functools.partial(lambda span, place: eig.at[place, span], span)
        ))
    eigens = tuple(range(blocks))
    for c in range(chunks):
        span = pl.ds(c * chunk, chunk)
        for own, full in ((nown, noi), (sown, see)):
            gathers.append((
                own.at[span],
                functools.partial(lambda full, span, place: full.at[place, span], full, span),
            ))
    stages = [0] * len(gathers)

    def hop(number, stage):
        own, full = gathers[number]
        sems = lambda way: (hsend.at[number, stage, way], hrecv.at[number, stage, way])

        def send(way, origin, other):
            src = own if stage == 0 else full(origin)
            slab.copy(src, full(origin), *sems(way), other).start()

        @pl.when((slab.me + 1 < slabs) & (slab.me >= stage))
        def _():
            send(0, slab.me - stage, slab.me + 1)

        @pl.when((slab.me >= 1) & (slab.me + stage < slabs))
        def _():
            send(1, slab.me + stage, slab.me - 1)

    def halted(number, stage, way):
        own, full = gathers[number]
        return slab.copy(
            own, full(slab.me), hsend.at[number, stage, way], hrecv.at[number, stage, way],
            slab.peer(1),
        )

    def landed(number, stage):
        @pl.when(slab.me >= 1 + stage)
        def _():
            halted(number, stage, 0).wait_recv()

        @pl.when(slab.me + 1 + stage < slabs)
        def _():
            halted(number, stage, 1).wait_recv()

    def left(number, stage):
        @pl.when((slab.me + 1 < slabs) & (slab.me >= stage))
        def _():
            halted(number, stage, 0).wait_send()

        @pl.when((slab.me >= 1) & (slab.me + stage < slabs))
        def _():
            halted(number, stage, 1).wait_send()

    def relay(*numbers):
        for number in numbers:
            stage = stages[number]
            if stage + 1 < slabs:
                landed(number, stage)
                if stage + 2 < slabs:
                    hop(number, stage + 1)
                stages[number] = stage + 1

    def complete(*numbers):
        for _ in range(slabs - 1):
            relay(*numbers)

    def of_rows(c):
        return (blocks + 2 * c, blocks + 2 * c + 1)

    def xcopy(number, slot, step, view):
        other = pencil.peer(step)
        return pencil.copy(
            view(put[number % 2], other), view(got[number], pencil.me),
            xsend.at[number, slot, step], xrecv.at[number, slot, step], other,
        )

    def xself(number, slot, view):
        return pltpu.make_async_copy(
            view(put[number % 2], pencil.me), view(got[number], pencil.me), xown.at[number, slot]
        )

    def by_rows(group):
        return lambda ref, place: ref.at[place, :, pl.ds(*group)]

    def by_part(b):
        return lambda ref, place: ref.at[place, pl.ds(b * block, block)]

    def xfinish(number, views):
        for slot, view in enumerate(views):
            for step in range(1, pencils):
                xcopy(number, slot, step, view).wait()
            xself(number, slot, view).wait()

    def first_stage(j, real, imag):
        length = real.shape[1]
        data = split(jnp.concatenate((real, imag), axis=1))
        first = dot3((fx[0], fx[1]), data, ((1,), (1,)))
        first = jnp.concatenate((first[:length], first[length:]), axis=1)
        for q in range(pencils):
            tmp[j, q] = first[q * part : (q + 1) * part]

    def emit(number, slot, group):
        span, count = pl.ds(*group), group[1]

        def one_block(q):
            data = jnp.concatenate([tmp[j, q] for j in range(count)], axis=0)
            out = dot3(split(data), (fz[0], fz[1]))
            out = jnp.stack([out[j * part : (j + 1) * part] for j in range(count)])
            put[number % 2][q, :, span] = jnp.swapaxes(out, 0, 1)

        def body(step, carry):
            one_block(pencil.peer(step))
            xcopy(number, slot, step, by_rows(group)).start()
            return carry

        lax.fori_loop(1, pencils, body, 0, unroll=QU)
        one_block(pencil.me)
        xself(number, slot, by_rows(group)).start()

    def absorb(number, group):
        span, count = pl.ds(*group), group[1]

        def body(q, carry):
            data = jnp.swapaxes(got[number][q, :, span], 0, 1)
            data = jnp.concatenate([data[j] for j in range(count)], axis=0)
            out = dot3(split(data), (gz[0], gz[1]))
            for j in range(count):
                tmp[j, q] = out[j * part : (j + 1) * part]
            return carry

        lax.fori_loop(0, pencils, body, 0, unroll=QU)

    def plane_back(j):
        first = jnp.concatenate([tmp[j, q] for q in range(pencils)], axis=0)
        first = jnp.concatenate((first[:, :nz], first[:, nz:]), axis=0)
        plane = dot3(split(first), (gx[0], gx[1]), ((0,), (0,)))
        return plane[:, :nx], plane[:, nx:]

    def lines(ref, y):
        return jnp.concatenate([ref[s, y] for s in range(slabs)], axis=0)

    def plane(ref, y, c):
        return jnp.concatenate([ref[s, y, c] for s in range(slabs)], axis=0)

    def store(ref, y, values):
        for c in range(2):
            for s in range(slabs):
                ref[s, y, c] = values[c][s * depth : (s + 1) * depth]

    def middle(number, after=None):
        def body(b, carry):
            for a2 in range(0, block, 2):
                spots = range(a2, min(a2 + 2, block))
                halves_of = []
                for a in spots:
                    data = jnp.concatenate(
                        [got[number][q, b * block + a] for q in range(pencils)], axis=0)
                    halves_of.append(jnp.concatenate((data[:, :nz], data[:, nz:]), axis=0))
                spec = dot3((fy[0], fy[1]), split(jnp.concatenate(halves_of, axis=1)))
                eigen = jnp.concatenate([
                    jnp.concatenate([eig[s, b * block + a] for s in range(slabs)], axis=0)
                    for a in spots], axis=1)
                spec = spec * jnp.concatenate((eigen, eigen), axis=0)
                back = dot3((gy[0], gy[1]), split(spec))
                ny = back.shape[0] // 2
                for k, a in enumerate(spots):
                    mine = back[:, k * nz : (k + 1) * nz]
                    mine = jnp.concatenate((mine[:ny], mine[ny:]), axis=1)
                    for q in range(pencils):
                        put[(number + 1) % 2][q, b * block + a] = mine[q * ys : (q + 1) * ys]
            for step in range(1, pencils):
                xcopy(number + 1, b, step, by_part(b)).start()
            xself(number + 1, b, by_part(b)).start()
            return carry

        lax.fori_loop(0, blocks, body, 0)

    def advance(number, old, new, target, which, ready=None):
        for slot, group in enumerate(groups):
            start_row, count = group
            absorb(number, group)
            if ready is not None:
                ready(start_row // chunk)

            def body(j, carry):
                y = start_row + j
                found = plane_back(j)
                mask, shift = lines(see, y), lines(noi, y) - SHIFT
                values = tuple(
                    (mask * t + shift * plane(old, y, k)) * (1.0 / SCALE)
                    for k, t in enumerate(found)
                )
                store(new, y, values)
                first_stage(j, *values)
                return carry

            lax.fori_loop(0, count, body, 0, unroll=YU)
            emit(number + 1, slot, group)
            start(zcopies(which, slot, *group, new, target))

    def turn(c):
        for load in naturals[c]:
            load.wait()
        rows_of = pl.ds(c * chunk, chunk)

        def body(k, carry):
            deep = pl.ds(pl.multiple_of(k * tile, tile), tile)
            mask = jnp.swapaxes(snat[deep, rows_of], 0, 1).astype(F32)
            sown[rows_of, deep] = mask
            nown[rows_of, deep] = jnp.swapaxes(nnat[deep, rows_of], 0, 1)
            for i in range(columns):
                values = jnp.swapaxes(nat[i, deep, rows_of], 0, 1)
                p0[i // 2, rows_of, i % 2, deep] = values
                if odd:
                    wa[i, rows_of, 0, deep] = values * mask
                    wa[i, rows_of, 1, deep] = jnp.zeros_like(values)
                else:
                    wa[i // 2, rows_of, i % 2, deep] = values * mask
            return carry

        lax.fori_loop(0, depths, body, 0)

    pieces = ys // piece
    met()
    for number in eigens:
        hop(number, 0)
    for c in range(chunks):
        turn(c)
        for k in range(c * chunk // piece, (c + 1) * chunk // piece):
            start(zcopies(0, k, k * piece, piece, wa, w0))
    own_loads = [
        brought(0, spectrum, eig.at[slab.me]), brought(1, nown, noi.at[slab.me]),
        brought(2, sown, see.at[slab.me]),
    ]
    start(own_loads)
    relay(*eigens)
    for number in of_rows(0):
        hop(number, 0)
    for load in loads:
        load.wait()
    for slot, (row, count) in enumerate(enter_groups):
        for k in range(row // piece, (row + count) // piece):
            finish(zcopies(0, k, k * piece, piece, wa, w0))

            def enter(j, carry):
                y = k * piece + j
                first_stage(y - row, plane(w0, y, 0), plane(w0, y, 1))
                return carry

            lax.fori_loop(0, piece, enter, 0, unroll=YU)
        emit(0, slot, (row, count))
    complete(*eigens)
    for c in range(1, chunks):
        for number in of_rows(c):
            hop(number, 0)
    finish(own_loads)
    xfinish(0, [by_rows(group) for group in enter_groups])
    middle(0)
    for _ in range(2):
        for c in range(chunks):
            relay(*of_rows(c))
    xfinish(1, [by_part(b) for b in range(blocks)])
    advance(1, w0, wa, x1, 1, lambda c: complete(*of_rows(c)))
    xfinish(2, [by_rows(group) for group in groups])
    middle(2)
    xfinish(3, [by_part(b) for b in range(blocks)])
    advance(3, wa, w0, x2, 2)
    xfinish(4, [by_rows(group) for group in groups])
    middle(4)
    for slot, group in enumerate(groups):
        finish(zcopies(1, slot, *group, wa, x1))
    xfinish(5, [by_part(b) for b in range(blocks)])
    for group in [(row, chunk) for row in range(0, ys, chunk)]:
        absorb(5, group)

        for row in range(group[0], sum(group), piece):
            def leave(j, carry):
                store(wa, row + j, plane_back(row - group[0] + j))
                return carry

            lax.fori_loop(0, piece, leave, 0, unroll=YU)
            start(zcopies(3, row // piece, row, piece, wa, x3))

    def tiles(step, row):
        y = row + step // depths
        return y, pl.ds(pl.multiple_of(step % depths * tile, tile), tile)

    pairs = [(i, j) for i in range(columns) for j in range(i, columns)]
    zero = tuple(jnp.zeros((tile, nx), F32) for _ in pairs)
    lane = lax.broadcasted_iota(jnp.int32, stat.shape, 1)

    def at(ref, i, y, z):
        return ref[i, y, 0, z] if odd else ref[i // 2, y, i % 2, z]

    def base(ref, i, y, z):
        return ref[i // 2, y, i % 2, z]

    def note(moment, sums):
        for total, (i, j) in zip(sums, pairs):
            row = jnp.sum(total, axis=0, keepdims=True)
            rows[pl.ds(i * columns + j, 1)] = row
            if i != j:
                rows[pl.ds(j * columns + i, 1)] = row
        found = stat[...]
        for i in range(columns):
            column = jnp.sum(rows[pl.ds(i * columns, columns)], axis=1, keepdims=True)
            found = jnp.where(lane == moment * columns + i, column, found)
        stat[...] = found

    def moment(number, left_of, right_of):
        def body(step, sums):
            y, z = tiles(step, 0)
            lefts = [left_of(i, y, z) for i in range(columns)]
            rights = lefts if right_of is left_of else [right_of(i, y, z) for i in range(columns)]
            return tuple(s + lefts[i] * rights[j] for s, (i, j) in zip(sums, pairs))

        note(number, lax.fori_loop(0, ys * depths, body, zero))

    stat[...] = jnp.zeros(stat.shape, F32)
    for slot, group in enumerate(groups):
        finish(zcopies(2, slot, *group, w0, x2))

    def shape_basis(step, carry):
        y, z = tiles(step, 0)
        mask = sown[y, z] > 0
        factor = (nown[y, z] - SHIFT) * (1.0 / SCALE)
        for i in range(columns):
            once = factor * base(p0, i, y, z)
            place = (i, y, 0, z) if odd else (i // 2, y, i % 2, z)
            x1[place] = jnp.where(mask, x1[place], once)
            x2[place] = jnp.where(mask, x2[place], factor * once)
        return carry

    lax.fori_loop(0, ys * depths, shape_basis, 0)
    outs = [pltpu.make_async_copy(x1, p1_o, lsem.at[0]), pltpu.make_async_copy(x2, p2_o, lsem.at[1])]
    start(outs)
    of0, of1, of2 = (functools.partial(f, r) for f, r in ((base, p0), (at, x1), (at, x2)))
    for number, (l, r) in enumerate(((of0, of0), (of0, of1), (of1, of1), (of1, of2), (of2, of2))):
        moment(number, l, r)
    sums = zero
    for k in range(pieces):
        finish(zcopies(3, k, k * piece, piece, wa, x3))

        def last(step, sums):
            y, z = tiles(step, k * piece)
            mask = sown[y, z] * (1.0 / SCALE)
            factor = (nown[y, z] - SHIFT) * (1.0 / SCALE)
            lefts, rights = [], []
            for i in range(columns):
                place = (i, y, 0, z) if odd else (i // 2, y, i % 2, z)
                lefts.append(x2[place])
                rights.append(mask * x3[place] + factor * lefts[-1])
                x3[place] = rights[-1]
            return tuple(s + lefts[i] * rights[j] for s, (i, j) in zip(sums, pairs))

        sums = lax.fori_loop(0, piece * depths, last, sums)
    note(5, sums)
    out = pltpu.make_async_copy(x3, u2_o, lsem.at[2])
    out.start()
    for number in range(len(gathers)):
        for stage in range(slabs - 1):
            left(number, stage)
    part_sum[...] = spread(pencil, stat, one, s1, r1)
    found = spread(slab, part_sum, two, s2, r2)
    c_ref[...], fine = small(found, columns)
    ok_ref[0, 0] = jnp.min(fine)
    finish(outs)
    out.wait()


def krylov(right, spectrum, noise, seen, tables):
    sizes = {name: lax.axis_size(name) for name in ("slab", "pencil")}
    slabs, pencils = sizes["slab"], sizes["pencil"]
    columns, depth, ys, nx = right.shape
    quads = columns // 2
    part, below, nz = spectrum.shape
    wide = 2 * nz
    chunk = 8 if ys % 8 == 0 else ys
    block = min(4, part)
    piece, half = min(2, chunk), max(chunk // 2, 1)
    planes = (slabs, ys, 2, depth, nx)
    gathered = (slabs, ys, depth, nx)
    sent = (pencils, part, ys, wide)
    whole_groups = [(row, chunk) for row in range(0, ys, chunk)]
    enter_groups = whole_groups[:-1] + [(ys - chunk, chunk - half)]
    enter_groups += [(row, piece) for row in range(ys - half, ys, piece)]
    groups = [(row, half) for row in range(0, chunk, half)] + whole_groups[1:]
    slots = max(len(enter_groups), len(groups), part // block)
    chunks = ys // chunk
    any_space = pl.BlockSpec(memory_space=pl.ANY)
    vmem = pl.BlockSpec(memory_space=pltpu.VMEM)
    dma = pltpu.SemaphoreType.DMA
    tile = (columns, 128)
    scratch = (
        [pltpu.VMEM(planes, F32)] * 5
        + [pltpu.VMEM((slabs,) + spectrum.shape, F32)]
        + [pltpu.VMEM(gathered, F32)] * 2
        + [[pltpu.VMEM(sent, F32)] * 2, [pltpu.VMEM(sent, F32)] * 6]
        + [pltpu.VMEM((chunk, pencils, part, wide), F32)]
        + [pltpu.VMEM((quads, ys, 2, depth, nx), F32)]
        + [pltpu.VMEM((ys, depth, nx), F32)] * 2
        + [pltpu.VMEM(v.shape, v.dtype) for v in (right, noise, seen)]
        + [pltpu.VMEM(t.shape, BF16) for t in tables]
        + [pltpu.VMEM((columns * columns, nx), F32), pltpu.VMEM(tile, F32)]
        + total_scratch(sizes, tile)[:3]
        + [dma((6, slots, pencils))] * 2 + [dma((6, slots))]
        + [dma((4, ys // piece, slabs))] * 2 + [dma((4, ys // piece))]
        + [dma((part // block + 2 * chunks, slabs, 2))] * 2 + [dma((4 * chunks + 6,))]
        + total_scratch(sizes, tile)[3:]
    )
    return pl.pallas_call(
        functools.partial(krylov_kernel, sizes, (
            chunk, block, piece, slabs == columns, enter_groups, groups)),
        in_specs=[any_space] * 10,
        out_specs=(any_space,) * 3 + (vmem, pl.BlockSpec(memory_space=pltpu.SMEM)),
        out_shape=(jax.ShapeDtypeStruct(planes, F32),) * 3 + (
            jax.ShapeDtypeStruct((ITERS * columns, columns), F32),
            jax.ShapeDtypeStruct((1, 1), F32),
        ),
        scratch_shapes=scratch,
        cost_estimate=pl.CostEstimate(flops=2**33, bytes_accessed=2**26, transcendentals=0),
        compiler_params=pltpu.CompilerParams(
            collective_id=0, has_side_effects=True, vmem_limit_bytes=60 * 2**20
        ),
    )(right, spectrum, noise, seen, *tables)


def mixed_kernel(odd, u_ref, v_ref, p0, p1, p2, p3, o_ref):
    quads, ys, _, depth, nx = p0.shape
    columns = 2 * quads
    tile = min(8, depth)
    pairs = [(i, j) for i in range(columns) for j in range(i, columns)]

    def body(step, sums):
        y, z = step // (depth // tile), pl.ds(pl.multiple_of(step % (depth // tile) * tile, tile), tile)
        tiles = [p0[i // 2, y, i % 2, z] for i in range(columns)]
        for ref in (p1, p2, p3):
            for i in range(columns):
                tiles.append(ref[i, y, 0, z] if odd else ref[i // 2, y, i % 2, z])
        left, right = (
            [sum(t * c_ref[k, i] for k, t in enumerate(tiles)) for i in range(columns)]
            for c_ref in (u_ref, v_ref)
        )
        return tuple(s + left[i] * right[j] for s, (i, j) in zip(sums, pairs))

    zero = jnp.zeros((tile, nx), F32)
    sums = lax.fori_loop(0, ys * (depth // tile), body, (zero,) * len(pairs))
    for total, (i, j) in zip(sums, pairs):
        row = jnp.sum(total, axis=0, keepdims=True)
        o_ref[pl.ds(i * columns + j, 1)] = row
        if i != j:
            o_ref[pl.ds(j * columns + i, 1)] = row


def recurrences(odd, basis):
    columns = 2 * basis[0].shape[0]

    def gram(u, v):
        wide = [
            jnp.pad(c.reshape(-1, columns), ((0, (ITERS + 1 - len(c)) * columns), (0, 0)))
            for c in (u, v)
        ]
        rows = pl.pallas_call(
            functools.partial(mixed_kernel, odd),
            in_specs=[pl.BlockSpec(memory_space=pltpu.SMEM)] * 2
            + [pl.BlockSpec(memory_space=pltpu.VMEM)] * 4,
            out_shape=jax.ShapeDtypeStruct((columns * columns, basis[0].shape[-1]), F32),
        )(*wide, *basis)
        return total_of(jnp.sum(rows, axis=1).reshape(columns, columns))

    def operator(c):
        zero = jnp.zeros((1, columns, columns), F32)
        return SHIFT * jnp.concatenate((c, zero)) + SCALE * jnp.concatenate((zero, c))

    def longer(c):
        return jnp.concatenate((c, jnp.zeros((1, columns, columns), F32)))

    residual = direction = answer = jnp.eye(columns, dtype=F32)[None]
    answer = 0.0 * answer
    gamma = gram(residual, residual)
    for iteration in range(ITERS):
        image = operator(direction)
        alpha = solve(gram(direction, image), gamma)
        answer = answer + jnp.einsum("kij,jp->kip", direction, alpha, precision=precise)
        if iteration + 1 < ITERS:
            residual = longer(residual) - jnp.einsum("kij,jp->kip", image, alpha, precision=precise)
            gamma_next = gram(residual, residual)
            beta = solve(gamma, gamma_next)
            direction = residual + longer(
                jnp.einsum("kij,jp->kip", direction, beta, precision=precise)
            )
            answer = longer(answer)
            gamma = gamma_next
    return answer.reshape(-1, columns)


def local(right_sides, spectrum, noise_var, observed):
    columns, depth, ys, nx = right_sides.shape
    slabs, pencils = lax.axis_size("slab"), lax.axis_size("pencil")
    nz, ny = depth * slabs, ys * pencils
    quads = columns // 2
    odd = slabs == columns

    fx, gx = halves(embed(nx, True)), halves(embed(nx, False).T)
    fz, gz = halves(embed(nz, True).T), halves(embed(nz, False).T)
    fy, gy = halves(embed(ny, True)), halves(embed(ny, False, 1.0 / (nx * ny * nz)))
    tables = [jnp.asarray(t) for t in (fx, fz, gx, gz, fy, gy)]
    p1, p2, u2, coefficients, fine = krylov(right_sides, spectrum, noise_var, observed, tables)

    def slow():
        field = jnp.transpose(right_sides.reshape(quads, 2, depth, ys, nx), (0, 3, 1, 2, 4))
        return recurrences(odd, (field, p1, p2, u2))

    coefficients = lax.cond(
        fine[0, 0] > 0.5, lambda: coefficients, slow
    )
    tile = min(8, depth)
    rows = ys
    planes = pl.BlockSpec((slabs, rows, 2, tile, nx), lambda i, j: (0, j, 0, i, 0))
    natural = pl.BlockSpec((columns, tile, rows, nx), lambda i, j: (0, i, j, 0))
    return tuple(pl.pallas_call(
        functools.partial(final_kernel, odd),
        grid=(depth // tile, ys // rows),
        in_specs=[pl.BlockSpec(memory_space=pltpu.SMEM), natural, planes, planes],
        out_specs=(natural, pl.BlockSpec((tile, rows, nx), lambda i, j: (i, j, 0))),
        out_shape=(
            jax.ShapeDtypeStruct(right_sides.shape, F32),
            jax.ShapeDtypeStruct((depth, ys, nx), F32),
        ),
    )(coefficients, right_sides, p1, p2))


def solution(mesh):
    in_specs = (
        P(None, "slab", "pencil", None),
        P("pencil", "slab", None),
        P("slab", "pencil", None),
        P("slab", "pencil", None),
    )
    out_specs = (P(None, "slab", "pencil", None), P("slab", "pencil", None))
    return jax.shard_map(local, mesh=mesh, in_specs=in_specs, out_specs=out_specs, check_vma=False)
```

```python
import functools

import jax
import jax.numpy as jnp
import numpy as np
from jax import lax
from jax.experimental import pallas as pl
from jax.experimental.pallas import tpu as pltpu
from jax.sharding import PartitionSpec as P

ITERS = 3
SHIFT = 8.0
SCALE = 8.0
FLOOR = 1e-2
F32 = jnp.float32
BF16 = jnp.bfloat16

precise = lax.Precision.HIGHEST


def embed(length, forward, scale=1.0):
    points = np.arange(length)
    angles = (points[:, None] * points[None, :] % length) * (2.0 * np.pi / length)
    cosine, sine = np.cos(angles) * scale, np.sin(angles) * scale
    if not forward:
        sine = -sine
    return np.block([[cosine, sine], [-sine, cosine]])


def halves(table):
    table = np.asarray(table, np.float32)
    high = table.astype(BF16)
    low = (table - high.astype(np.float32)).astype(BF16)
    return np.stack((high, low))


def split(values):
    high = values.astype(BF16)
    return high, (values - high.astype(F32)).astype(BF16)


def dot3(left, right, dims=((1,), (0,))):
    mul = functools.partial(
        lax.dot_general, dimension_numbers=(dims, ((), ())), preferred_element_type=F32
    )
    return mul(left[0], right[0]) + (mul(left[1], right[0]) + mul(left[0], right[1]))


def solve(matrix, right_hand):
    size = matrix.shape[0]
    both = jnp.concatenate((0.5 * (matrix + matrix.T), right_hand), axis=1)
    place = lax.broadcasted_iota(jnp.int32, both.shape, 0)
    for i in range(size):
        row = both[i : i + 1] / both[i : i + 1, i : i + 1]
        both = jnp.where(place == i, row, both - both[:, i : i + 1] * row)
    return both[:, size:]


def small(moments, columns):
    span = ITERS * columns
    pick = lambda first, count: moments[:, first * columns : first * columns + count]
    both = jnp.concatenate([
        jnp.concatenate((SHIFT * pick(j, span) + SCALE * pick(j + 1, span), pick(j, columns)), axis=1)
        for j in range(ITERS)
    ], axis=0)
    place = lax.broadcasted_iota(jnp.int32, both.shape, 0)
    fine = jnp.ones((1, columns), F32)
    old = both
    for i in range(span):
        pivot = both[i : i + 1, i : i + 1]
        fine = jnp.where(pivot > FLOOR * old[i : i + 1, i : i + 1], fine, 0.0)
        row = both[i : i + 1] / pivot
        both = jnp.where(place == i, row, both - both[:, i : i + 1] * row)
    return both[:, span:], fine


def final_kernel(odd, c_ref, right, p1, p2, x_ref, g_ref):
    columns, tile, ys, _ = right.shape
    chunk = 8 if ys % 8 == 0 else ys

    def at(ref, i, y):
        return ref[i, pl.ds(y, chunk), 0] if odd else ref[i // 2, pl.ds(y, chunk), i % 2]

    for y in range(0, ys, chunk):
        rows = pl.ds(y, chunk)

        def column(p):
            found = 0.0
            for k, ref in ((1, p1), (2, p2)):
                for i in range(columns):
                    found = found + at(ref, i, y) * c_ref[k * columns + i, p]
            found = jnp.swapaxes(found, 0, 1)
            for i in range(columns):
                found = found + right[i, :, rows] * c_ref[i, p]
            x_ref[p, :, rows] = found
            return found

        def body(p, grad):
            return grad - right[p, :, rows] * column(p) * (0.5 / (columns - 1))

        first = column(0)
        g_ref[:, rows] = lax.fori_loop(1, columns, body, 0.5 * first * first)


QU, YU = 4, 4
MESH = pl.DeviceIdType.MESH


class Group:
    def __init__(self, sizes, axis):
        self.axis, self.size = axis, sizes[axis]
        self.names = tuple(sizes)
        self.place = {name: lax.axis_index(name) for name in sizes}
        self.me = self.place[axis]

    def peer(self, step):
        return lax.rem(self.me + step, self.size)

    def device(self, other):
        return tuple(other if name == self.axis else self.place[name] for name in self.names)

    def copy(self, src, dst, send, recv, other):
        return pltpu.make_async_remote_copy(
            src_ref=src, dst_ref=dst, send_sem=send, recv_sem=recv,
            device_id=self.device(other), device_id_type=MESH,
        )


def greet(groups):
    barrier = pltpu.get_barrier_semaphore()
    total = 0
    for group in groups:
        for step in range(1, group.size):
            pl.semaphore_signal(
                barrier, inc=1, device_id=group.device(group.peer(step)), device_id_type=MESH
            )
            total += 1
    return lambda: pl.semaphore_wait(barrier, total)


def spread(group, source, target, send, recv):
    copies = []
    for step in range(1, group.size):
        copy = group.copy(
            source, target.at[group.me], send.at[step], recv.at[step], group.peer(step)
        )
        copy.start()
        copies.append(copy)
    target[group.me] = source[...]
    for copy in copies:
        copy.wait()
    total = target[0]
    for place in range(1, group.size):
        total = total + target[place]
    return total


def total_kernel(sizes, v_ref, o_ref, part, one, two, send, recv, send2, recv2):
    slab, pencil = Group(sizes, "slab"), Group(sizes, "pencil")
    greet((slab, pencil))()
    part[...] = spread(pencil, v_ref, one, send, recv)
    o_ref[...] = spread(slab, part, two, send2, recv2)


def total_scratch(sizes, shape):
    return [
        pltpu.VMEM(shape, F32),
        pltpu.VMEM((sizes["pencil"],) + shape, F32),
        pltpu.VMEM((sizes["slab"],) + shape, F32),
        pltpu.SemaphoreType.DMA((sizes["pencil"],)),
        pltpu.SemaphoreType.DMA((sizes["pencil"],)),
        pltpu.SemaphoreType.DMA((sizes["slab"],)),
        pltpu.SemaphoreType.DMA((sizes["slab"],)),
    ]


def total_of(matrix):
    sizes = {name: lax.axis_size(name) for name in ("slab", "pencil")}
    rows, columns = matrix.shape
    wide = jnp.pad(matrix, ((0, 0), (0, 128 - columns)))
    found = pl.pallas_call(
        functools.partial(total_kernel, sizes),
        in_specs=[pl.BlockSpec(memory_space=pltpu.VMEM)],
        out_specs=pl.BlockSpec(memory_space=pltpu.VMEM),
        out_shape=jax.ShapeDtypeStruct(wide.shape, F32),
        scratch_shapes=total_scratch(sizes, wide.shape),
        compiler_params=pltpu.CompilerParams(collective_id=1, has_side_effects=True),
    )(wide)
    return found[:, :columns]


def krylov_kernel(
    sizes, plan,
    right, spectrum, noise, seen, fx_h, fz_h, gx_h, gz_h, fy_h, gy_h,
    p1_o, p2_o, u2_o, c_ref, ok_ref,
    w0, wa, x1, x2, x3, eig, noi, see, put, got, tmp, p0, nown, sown, nat, nnat, snat,
    fx, fz, gx, gz, fy, gy, rows, stat, part_sum, one, two,
    xsend, xrecv, xown, zsend, zrecv, zown, hsend, hrecv, lsem, s1, r1, s2, r2,
):
    slab, pencil = Group(sizes, "slab"), Group(sizes, "pencil")
    slabs, pencils = slab.size, pencil.size
    _, ys, _, depth, nx = w0.shape
    part, wide = got[0].shape[1], got[0].shape[3]
    nz = wide // 2
    chunk, block, piece, odd, enter_groups, groups = plan
    chunks, blocks = ys // chunk, part // block
    columns = right.shape[0]
    tile = min(8, depth)
    depths = depth // tile

    def brought(slot, src, dst):
        return pltpu.make_async_copy(src, dst, lsem.at[slot])

    met = greet((slab, pencil))
    naturals = []
    for c in range(chunks):
        span = pl.ds(c * chunk, chunk)
        naturals.append([
            brought(4 * c, seen.at[:, span], snat.at[:, span]),
            brought(4 * c + 1, right.at[:, :, span], nat.at[:, :, span]),
            brought(4 * c + 2, noise.at[:, span], nnat.at[:, span]),
        ])
        for load in naturals[-1]:
            load.start()
    tables = ((fx_h, fx), (fz_h, fz), (gx_h, gx), (gz_h, gz), (fy_h, fy), (gy_h, gy))
    loads = [brought(4 * chunks + i, a, b) for i, (a, b) in enumerate(tables)]
    for load in loads:
        load.start()

    def zrows(ref, y, count):
        return ref.at[:, pl.ds(y, count)]

    def zcopies(number, slot, y, count, src, dst):
        made = []
        for step in range(1, slabs):
            other = slab.peer(step)
            made.append(slab.copy(
                src.at[other, pl.ds(y, count)], dst.at[slab.me, pl.ds(y, count)],
                zsend.at[number, slot, step], zrecv.at[number, slot, step], other,
            ))
        made.append(pltpu.make_async_copy(
            src.at[slab.me, pl.ds(y, count)], dst.at[slab.me, pl.ds(y, count)],
            zown.at[number, slot],
        ))
        return made

    def start(copies):
        for copy in copies:
            copy.start()

    def finish(copies):
        for copy in copies:
            copy.wait()

    gathers = []
    for b in range(blocks):
        span = pl.ds(b * block, block)
        gathers.append((
            spectrum.at[span], functools.partial(lambda span, place: eig.at[place, span], span)
        ))
    eigens = tuple(range(blocks))
    for c in range(chunks):
        span = pl.ds(c * chunk, chunk)
        for own, full in ((nown, noi), (sown, see)):
            gathers.append((
                own.at[span],
                functools.partial(lambda full, span, place: full.at[place, span], full, span),
            ))
    stages = [0] * len(gathers)

    def hop(number, stage):
        own, full = gathers[number]
        sems = lambda way: (hsend.at[number, stage, way], hrecv.at[number, stage, way])

        def send(way, origin, other):
            src = own if stage == 0 else full(origin)
            slab.copy(src, full(origin), *sems(way), other).start()

        @pl.when((slab.me + 1 < slabs) & (slab.me >= stage))
        def _():
            send(0, slab.me - stage, slab.me + 1)

        @pl.when((slab.me >= 1) & (slab.me + stage < slabs))
        def _():
            send(1, slab.me + stage, slab.me - 1)

    def halted(number, stage, way):
        own, full = gathers[number]
        return slab.copy(
            own, full(slab.me), hsend.at[number, stage, way], hrecv.at[number, stage, way],
            slab.peer(1),
        )

    def landed(number, stage):
        @pl.when(slab.me >= 1 + stage)
        def _():
            halted(number, stage, 0).wait_recv()

        @pl.when(slab.me + 1 + stage < slabs)
        def _():
            halted(number, stage, 1).wait_recv()

    def left(number, stage):
        @pl.when((slab.me + 1 < slabs) & (slab.me >= stage))
        def _():
            halted(number, stage, 0).wait_send()

        @pl.when((slab.me >= 1) & (slab.me + stage < slabs))
        def _():
            halted(number, stage, 1).wait_send()

    def relay(*numbers):
        for number in numbers:
            stage = stages[number]
            if stage + 1 < slabs:
                landed(number, stage)
                if stage + 2 < slabs:
                    hop(number, stage + 1)
                stages[number] = stage + 1

    def complete(*numbers):
        for _ in range(slabs - 1):
            relay(*numbers)

    def of_rows(c):
        return (blocks + 2 * c, blocks + 2 * c + 1)

    def xcopy(number, slot, step, view):
        other = pencil.peer(step)
        return pencil.copy(
            view(put[number % 2], other), view(got[number], pencil.me),
            xsend.at[number, slot, step], xrecv.at[number, slot, step], other,
        )

    def xself(number, slot, view):
        return pltpu.make_async_copy(
            view(put[number % 2], pencil.me), view(got[number], pencil.me), xown.at[number, slot]
        )

    def by_rows(group):
        return lambda ref, place: ref.at[place, :, pl.ds(*group)]

    def by_part(b):
        return lambda ref, place: ref.at[place, pl.ds(b * block, block)]

    def xfinish(number, views):
        for slot, view in enumerate(views):
            for step in range(1, pencils):
                xcopy(number, slot, step, view).wait()
            xself(number, slot, view).wait()

    def first_stage(j, real, imag):
        length = real.shape[1]
        data = split(jnp.concatenate((real, imag), axis=1))
        first = dot3((fx[0], fx[1]), data, ((1,), (1,)))
        first = jnp.concatenate((first[:length], first[length:]), axis=1)
        for q in range(pencils):
            tmp[j, q] = first[q * part : (q + 1) * part]

    def emit(number, slot, group):
        span, count = pl.ds(*group), group[1]

        def one_block(q):
            data = jnp.concatenate([tmp[j, q] for j in range(count)], axis=0)
            out = dot3(split(data), (fz[0], fz[1]))
            out = jnp.stack([out[j * part : (j + 1) * part] for j in range(count)])
            put[number % 2][q, :, span] = jnp.swapaxes(out, 0, 1)

        def body(step, carry):
            one_block(pencil.peer(step))
            xcopy(number, slot, step, by_rows(group)).start()
            return carry

        lax.fori_loop(1, pencils, body, 0, unroll=QU)
        one_block(pencil.me)
        xself(number, slot, by_rows(group)).start()

    def absorb(number, group):
        span, count = pl.ds(*group), group[1]

        def body(q, carry):
            data = jnp.swapaxes(got[number][q, :, span], 0, 1)
            data = jnp.concatenate([data[j] for j in range(count)], axis=0)
            out = dot3(split(data), (gz[0], gz[1]))
            for j in range(count):
                tmp[j, q] = out[j * part : (j + 1) * part]
            return carry

        lax.fori_loop(0, pencils, body, 0, unroll=QU)

    def plane_back(j):
        first = jnp.concatenate([tmp[j, q] for q in range(pencils)], axis=0)
        first = jnp.concatenate((first[:, :nz], first[:, nz:]), axis=0)
        plane = dot3(split(first), (gx[0], gx[1]), ((0,), (0,)))
        return plane[:, :nx], plane[:, nx:]

    def lines(ref, y):
        return jnp.concatenate([ref[s, y] for s in range(slabs)], axis=0)

    def plane(ref, y, c):
        return jnp.concatenate([ref[s, y, c] for s in range(slabs)], axis=0)

    def store(ref, y, values):
        for c in range(2):
            for s in range(slabs):
                ref[s, y, c] = values[c][s * depth : (s + 1) * depth]

    def middle(number, after=None):
        def body(b, carry):
            for a2 in range(0, block, 2):
                spots = range(a2, min(a2 + 2, block))
                halves_of = []
                for a in spots:
                    data = jnp.concatenate(
                        [got[number][q, b * block + a] for q in range(pencils)], axis=0)
                    halves_of.append(jnp.concatenate((data[:, :nz], data[:, nz:]), axis=0))
                spec = dot3((fy[0], fy[1]), split(jnp.concatenate(halves_of, axis=1)))
                eigen = jnp.concatenate([
                    jnp.concatenate([eig[s, b * block + a] for s in range(slabs)], axis=0)
                    for a in spots], axis=1)
                spec = spec * jnp.concatenate((eigen, eigen), axis=0)
                back = dot3((gy[0], gy[1]), split(spec))
                ny = back.shape[0] // 2
                for k, a in enumerate(spots):
                    mine = back[:, k * nz : (k + 1) * nz]
                    mine = jnp.concatenate((mine[:ny], mine[ny:]), axis=1)
                    for q in range(pencils):
                        put[(number + 1) % 2][q, b * block + a] = mine[q * ys : (q + 1) * ys]
            for step in range(1, pencils):
                xcopy(number + 1, b, step, by_part(b)).start()
            xself(number + 1, b, by_part(b)).start()
            return carry

        lax.fori_loop(0, blocks, body, 0)

    def advance(number, old, new, target, which, ready=None):
        for slot, group in enumerate(groups):
            start_row, count = group
            absorb(number, group)
            if ready is not None:
                ready(start_row // chunk)

            def body(j, carry):
                y = start_row + j
                found = plane_back(j)
                mask, shift = lines(see, y), lines(noi, y) - SHIFT
                values = tuple(
                    (mask * t + shift * plane(old, y, k)) * (1.0 / SCALE)
                    for k, t in enumerate(found)
                )
                store(new, y, values)
                first_stage(j, *values)
                return carry

            lax.fori_loop(0, count, body, 0, unroll=YU)
            emit(number + 1, slot, group)
            start(zcopies(which, slot, *group, new, target))

    def turn(c):
        for load in naturals[c]:
            load.wait()
        rows_of = pl.ds(c * chunk, chunk)

        def body(k, carry):
            deep = pl.ds(pl.multiple_of(k * tile, tile), tile)
            mask = jnp.swapaxes(snat[deep, rows_of], 0, 1).astype(F32)
            sown[rows_of, deep] = mask
            nown[rows_of, deep] = jnp.swapaxes(nnat[deep, rows_of], 0, 1)
            for i in range(columns):
                values = jnp.swapaxes(nat[i, deep, rows_of], 0, 1)
                p0[i // 2, rows_of, i % 2, deep] = values
                if odd:
                    wa[i, rows_of, 0, deep] = values * mask
                    wa[i, rows_of, 1, deep] = jnp.zeros_like(values)
                else:
                    wa[i // 2, rows_of, i % 2, deep] = values * mask
            return carry

        lax.fori_loop(0, depths, body, 0)

    pieces = ys // piece
    met()
    for number in eigens:
        hop(number, 0)
    for c in range(chunks):
        turn(c)
        for k in range(c * chunk // piece, (c + 1) * chunk // piece):
            start(zcopies(0, k, k * piece, piece, wa, w0))
    own_loads = [
        brought(0, spectrum, eig.at[slab.me]), brought(1, nown, noi.at[slab.me]),
        brought(2, sown, see.at[slab.me]),
    ]
    start(own_loads)
    relay(*eigens)
    for number in of_rows(0):
        hop(number, 0)
    for load in loads:
        load.wait()
    for slot, (row, count) in enumerate(enter_groups):
        for k in range(row // piece, (row + count) // piece):
            finish(zcopies(0, k, k * piece, piece, wa, w0))

            def enter(j, carry):
                y = k * piece + j
                first_stage(y - row, plane(w0, y, 0), plane(w0, y, 1))
                return carry

            lax.fori_loop(0, piece, enter, 0, unroll=YU)
        emit(0, slot, (row, count))
    complete(*eigens)
    for c in range(1, chunks):
        for number in of_rows(c):
            hop(number, 0)
    finish(own_loads)
    xfinish(0, [by_rows(group) for group in enter_groups])
    middle(0)
    for _ in range(2):
        for c in range(chunks):
            relay(*of_rows(c))
    xfinish(1, [by_part(b) for b in range(blocks)])
    advance(1, w0, wa, x1, 1, lambda c: complete(*of_rows(c)))
    xfinish(2, [by_rows(group) for group in groups])
    middle(2)
    xfinish(3, [by_part(b) for b in range(blocks)])
    advance(3, wa, w0, x2, 2)
    xfinish(4, [by_rows(group) for group in groups])
    middle(4)
    for slot, group in enumerate(groups):
        finish(zcopies(1, slot, *group, wa, x1))
    xfinish(5, [by_part(b) for b in range(blocks)])
    for group in [(row, chunk) for row in range(0, ys, chunk)]:
        absorb(5, group)

        for row in range(group[0], sum(group), piece):
            def leave(j, carry):
                store(wa, row + j, plane_back(row - group[0] + j))
                return carry

            lax.fori_loop(0, piece, leave, 0, unroll=YU)
            start(zcopies(3, row // piece, row, piece, wa, x3))

    def tiles(step, row):
        y = row + step // depths
        return y, pl.ds(pl.multiple_of(step % depths * tile, tile), tile)

    pairs = [(i, j) for i in range(columns) for j in range(i, columns)]
    zero = tuple(jnp.zeros((tile, nx), F32) for _ in pairs)
    lane = lax.broadcasted_iota(jnp.int32, stat.shape, 1)

    def at(ref, i, y, z):
        return ref[i, y, 0, z] if odd else ref[i // 2, y, i % 2, z]

    def base(ref, i, y, z):
        return ref[i // 2, y, i % 2, z]

    def note(moment, sums):
        for total, (i, j) in zip(sums, pairs):
            row = jnp.sum(total, axis=0, keepdims=True)
            rows[pl.ds(i * columns + j, 1)] = row
            if i != j:
                rows[pl.ds(j * columns + i, 1)] = row
        found = stat[...]
        for i in range(columns):
            column = jnp.sum(rows[pl.ds(i * columns, columns)], axis=1, keepdims=True)
            found = jnp.where(lane == moment * columns + i, column, found)
        stat[...] = found

    def moment(number, left_of, right_of):
        def body(step, sums):
            y, z = tiles(step, 0)
            lefts = [left_of(i, y, z) for i in range(columns)]
            rights = lefts if right_of is left_of else [right_of(i, y, z) for i in range(columns)]
            return tuple(s + lefts[i] * rights[j] for s, (i, j) in zip(sums, pairs))

        note(number, lax.fori_loop(0, ys * depths, body, zero))

    stat[...] = jnp.zeros(stat.shape, F32)
    for slot, group in enumerate(groups):
        finish(zcopies(2, slot, *group, w0, x2))

    def shape_basis(step, carry):
        y, z = tiles(step, 0)
        mask = sown[y, z] > 0
        factor = (nown[y, z] - SHIFT) * (1.0 / SCALE)
        for i in range(columns):
            once = factor * base(p0, i, y, z)
            place = (i, y, 0, z) if odd else (i // 2, y, i % 2, z)
            x1[place] = jnp.where(mask, x1[place], once)
            x2[place] = jnp.where(mask, x2[place], factor * once)
        return carry

    lax.fori_loop(0, ys * depths, shape_basis, 0)
    outs = [pltpu.make_async_copy(x1, p1_o, lsem.at[0]), pltpu.make_async_copy(x2, p2_o, lsem.at[1])]
    start(outs)
    of0, of1, of2 = (functools.partial(f, r) for f, r in ((base, p0), (at, x1), (at, x2)))
    for number, (l, r) in enumerate(((of0, of0), (of0, of1), (of1, of1), (of1, of2), (of2, of2))):
        moment(number, l, r)
    sums = zero
    for k in range(pieces):
        finish(zcopies(3, k, k * piece, piece, wa, x3))

        def last(step, sums):
            y, z = tiles(step, k * piece)
            mask = sown[y, z] * (1.0 / SCALE)
            factor = (nown[y, z] - SHIFT) * (1.0 / SCALE)
            lefts, rights = [], []
            for i in range(columns):
                place = (i, y, 0, z) if odd else (i // 2, y, i % 2, z)
                lefts.append(x2[place])
                rights.append(mask * x3[place] + factor * lefts[-1])
                x3[place] = rights[-1]
            return tuple(s + lefts[i] * rights[j] for s, (i, j) in zip(sums, pairs))

        sums = lax.fori_loop(0, piece * depths, last, sums)
    note(5, sums)
    out = pltpu.make_async_copy(x3, u2_o, lsem.at[2])
    out.start()
    for number in range(len(gathers)):
        for stage in range(slabs - 1):
            left(number, stage)
    part_sum[...] = spread(pencil, stat, one, s1, r1)
    found = spread(slab, part_sum, two, s2, r2)
    c_ref[...], fine = small(found, columns)
    ok_ref[0, 0] = jnp.min(fine)
    finish(outs)
    out.wait()


def krylov(right, spectrum, noise, seen, tables):
    sizes = {name: lax.axis_size(name) for name in ("slab", "pencil")}
    slabs, pencils = sizes["slab"], sizes["pencil"]
    columns, depth, ys, nx = right.shape
    quads = columns // 2
    part, below, nz = spectrum.shape
    wide = 2 * nz
    chunk = 8 if ys % 8 == 0 else ys
    block = min(8, part)
    piece, half = min(2, chunk), max(chunk // 2, 1)
    planes = (slabs, ys, 2, depth, nx)
    gathered = (slabs, ys, depth, nx)
    sent = (pencils, part, ys, wide)
    whole_groups = [(row, chunk) for row in range(0, ys, chunk)]
    enter_groups = whole_groups[:-1] + [(ys - chunk, chunk - half)]
    enter_groups += [(row, piece) for row in range(ys - half, ys, piece)]
    groups = [(row, half) for row in range(0, chunk, half)] + whole_groups[1:]
    slots = max(len(enter_groups), len(groups), part // block)
    chunks = ys // chunk
    any_space = pl.BlockSpec(memory_space=pl.ANY)
    vmem = pl.BlockSpec(memory_space=pltpu.VMEM)
    dma = pltpu.SemaphoreType.DMA
    tile = (columns, 128)
    scratch = (
        [pltpu.VMEM(planes, F32)] * 5
        + [pltpu.VMEM((slabs,) + spectrum.shape, F32)]
        + [pltpu.VMEM(gathered, F32)] * 2
        + [[pltpu.VMEM(sent, F32)] * 2, [pltpu.VMEM(sent, F32)] * 6]
        + [pltpu.VMEM((chunk, pencils, part, wide), F32)]
        + [pltpu.VMEM((quads, ys, 2, depth, nx), F32)]
        + [pltpu.VMEM((ys, depth, nx), F32)] * 2
        + [pltpu.VMEM(v.shape, v.dtype) for v in (right, noise, seen)]
        + [pltpu.VMEM(t.shape, BF16) for t in tables]
        + [pltpu.VMEM((columns * columns, nx), F32), pltpu.VMEM(tile, F32)]
        + total_scratch(sizes, tile)[:3]
        + [dma((6, slots, pencils))] * 2 + [dma((6, slots))]
        + [dma((4, ys // piece, slabs))] * 2 + [dma((4, ys // piece))]
        + [dma((part // block + 2 * chunks, slabs, 2))] * 2 + [dma((4 * chunks + 6,))]
        + total_scratch(sizes, tile)[3:]
    )
    return pl.pallas_call(
        functools.partial(krylov_kernel, sizes, (
            chunk, block, piece, slabs == columns, enter_groups, groups)),
        in_specs=[any_space] * 10,
        out_specs=(any_space,) * 3 + (vmem, pl.BlockSpec(memory_space=pltpu.SMEM)),
        out_shape=(jax.ShapeDtypeStruct(planes, F32),) * 3 + (
            jax.ShapeDtypeStruct((ITERS * columns, columns), F32),
            jax.ShapeDtypeStruct((1, 1), F32),
        ),
        scratch_shapes=scratch,
        cost_estimate=pl.CostEstimate(flops=2**33, bytes_accessed=2**26, transcendentals=0),
        compiler_params=pltpu.CompilerParams(
            collective_id=0, has_side_effects=True, vmem_limit_bytes=60 * 2**20
        ),
    )(right, spectrum, noise, seen, *tables)


def mixed_kernel(odd, u_ref, v_ref, p0, p1, p2, p3, o_ref):
    quads, ys, _, depth, nx = p0.shape
    columns = 2 * quads
    tile = min(8, depth)
    pairs = [(i, j) for i in range(columns) for j in range(i, columns)]

    def body(step, sums):
        y, z = step // (depth // tile), pl.ds(pl.multiple_of(step % (depth // tile) * tile, tile), tile)
        tiles = [p0[i // 2, y, i % 2, z] for i in range(columns)]
        for ref in (p1, p2, p3):
            for i in range(columns):
                tiles.append(ref[i, y, 0, z] if odd else ref[i // 2, y, i % 2, z])
        left, right = (
            [sum(t * c_ref[k, i] for k, t in enumerate(tiles)) for i in range(columns)]
            for c_ref in (u_ref, v_ref)
        )
        return tuple(s + left[i] * right[j] for s, (i, j) in zip(sums, pairs))

    zero = jnp.zeros((tile, nx), F32)
    sums = lax.fori_loop(0, ys * (depth // tile), body, (zero,) * len(pairs))
    for total, (i, j) in zip(sums, pairs):
        row = jnp.sum(total, axis=0, keepdims=True)
        o_ref[pl.ds(i * columns + j, 1)] = row
        if i != j:
            o_ref[pl.ds(j * columns + i, 1)] = row


def recurrences(odd, basis):
    columns = 2 * basis[0].shape[0]

    def gram(u, v):
        wide = [
            jnp.pad(c.reshape(-1, columns), ((0, (ITERS + 1 - len(c)) * columns), (0, 0)))
            for c in (u, v)
        ]
        rows = pl.pallas_call(
            functools.partial(mixed_kernel, odd),
            in_specs=[pl.BlockSpec(memory_space=pltpu.SMEM)] * 2
            + [pl.BlockSpec(memory_space=pltpu.VMEM)] * 4,
            out_shape=jax.ShapeDtypeStruct((columns * columns, basis[0].shape[-1]), F32),
        )(*wide, *basis)
        return total_of(jnp.sum(rows, axis=1).reshape(columns, columns))

    def operator(c):
        zero = jnp.zeros((1, columns, columns), F32)
        return SHIFT * jnp.concatenate((c, zero)) + SCALE * jnp.concatenate((zero, c))

    def longer(c):
        return jnp.concatenate((c, jnp.zeros((1, columns, columns), F32)))

    residual = direction = answer = jnp.eye(columns, dtype=F32)[None]
    answer = 0.0 * answer
    gamma = gram(residual, residual)
    for iteration in range(ITERS):
        image = operator(direction)
        alpha = solve(gram(direction, image), gamma)
        answer = answer + jnp.einsum("kij,jp->kip", direction, alpha, precision=precise)
        if iteration + 1 < ITERS:
            residual = longer(residual) - jnp.einsum("kij,jp->kip", image, alpha, precision=precise)
            gamma_next = gram(residual, residual)
            beta = solve(gamma, gamma_next)
            direction = residual + longer(
                jnp.einsum("kij,jp->kip", direction, beta, precision=precise)
            )
            answer = longer(answer)
            gamma = gamma_next
    return answer.reshape(-1, columns)


def local(right_sides, spectrum, noise_var, observed):
    columns, depth, ys, nx = right_sides.shape
    slabs, pencils = lax.axis_size("slab"), lax.axis_size("pencil")
    nz, ny = depth * slabs, ys * pencils
    quads = columns // 2
    odd = slabs == columns

    fx, gx = halves(embed(nx, True)), halves(embed(nx, False).T)
    fz, gz = halves(embed(nz, True).T), halves(embed(nz, False).T)
    fy, gy = halves(embed(ny, True)), halves(embed(ny, False, 1.0 / (nx * ny * nz)))
    tables = [jnp.asarray(t) for t in (fx, fz, gx, gz, fy, gy)]
    p1, p2, u2, coefficients, fine = krylov(right_sides, spectrum, noise_var, observed, tables)

    def slow():
        field = jnp.transpose(right_sides.reshape(quads, 2, depth, ys, nx), (0, 3, 1, 2, 4))
        return recurrences(odd, (field, p1, p2, u2))

    coefficients = lax.cond(
        fine[0, 0] > 0.5, lambda: coefficients, slow
    )
    tile = min(8, depth)
    rows = ys
    planes = pl.BlockSpec((slabs, rows, 2, tile, nx), lambda i, j: (0, j, 0, i, 0))
    natural = pl.BlockSpec((columns, tile, rows, nx), lambda i, j: (0, i, j, 0))
    return tuple(pl.pallas_call(
        functools.partial(final_kernel, odd),
        grid=(depth // tile, ys // rows),
        in_specs=[pl.BlockSpec(memory_space=pltpu.SMEM), natural, planes, planes],
        out_specs=(natural, pl.BlockSpec((tile, rows, nx), lambda i, j: (i, j, 0))),
        out_shape=(
            jax.ShapeDtypeStruct(right_sides.shape, F32),
            jax.ShapeDtypeStruct((depth, ys, nx), F32),
        ),
    )(coefficients, right_sides, p1, p2))


def solution(mesh):
    in_specs = (
        P(None, "slab", "pencil", None),
        P("pencil", "slab", None),
        P("slab", "pencil", None),
        P("slab", "pencil", None),
    )
    out_specs = (P(None, "slab", "pencil", None), P("slab", "pencil", None))
    return jax.shard_map(local, mesh=mesh, in_specs=in_specs, out_specs=out_specs, check_vma=False)
```
